256 devices in a mesh: groups: 2 (over y), bank: 16 (over z), freq: 4 (over x), seg: 2 (over core).
Axes of the slice: x: 4, y: 2, z: 16, core: 2. Of those that a mesh axis runs over, the one named last changes fastest.
The devices are a block of a 4x16x16 slice.
Arguments:
- coarse_spectra: bfloat16 [256, 2, 16384], P(('groups', 'seg', 'bank'), None, 'freq'), parts along dimension 0, may hold values from -6 to 6
- fine_spectra: bfloat16 [256, 2, 65536], P(('groups', 'seg', 'bank'), None, 'freq'), parts along dimension 0, may hold values from -6 to 6
- coarse_templates: bfloat16 [2, 2048, 16384], P(None, 'bank', 'freq'), may hold values from -6 to 6
- fine_templates: bfloat16 [2, 16, 64, 65536], P(None, 'bank', None, 'freq'), may hold values from -6 to 6
- coarse_weight: float32 [32768], P(('groups', 'freq')), parts along dimension 0, may hold values from 0.2 to 2
- fine_weight: float32 [131072], P(('groups', 'freq')), parts along dimension 0, may hold values from 0.2 to 2
- triggers: int32 [256, 2], P(('groups', 'seg')), parts along dimension 0, may hold values from 0 to 15, all different within a row; in each aligned block of 4 rows (0 to 3, 4 to 7, ...) at most 2 rows name the same one
- offsets: int32 [256, 2], P(('groups', 'seg')), parts along dimension 0, may hold values from 0 to 131056
Outputs:
- coarse_snr: float32 [2048, 256], P(('bank', 'freq'), ('groups', 'seg')), parts along dimension 1
- fine_snr: float32 [256, 2, 64], P(('groups', 'seg', 'bank'), None, 'freq'), parts along dimension 0
The draws below stay inside these ranges and needn't reach their ends.
There are 2 independent parts, one for each index of `groups`. The reference program is written for one: setup_inputs(seed, part) draws one part's arguments, and reference() takes and returns one part's arrays. A program takes and returns all parts, laid end to end along the dimension named above; an argument that names none is the same for every part. Nothing has to cross between parts.
Inputs may be any that keep to these rules, and one draw needn't show every extreme that they name: `triggers`: each segment names 2 different sub-banks. In each aligned block of 4 segments (the segments of one device along seg and bank) no sub-bank is named more than 2 times.
All inputs are finite; a program needn't handle non-finite values.
Results may differ from the reference program's by a relative error of at most 0.0021.
Values may be sent and summed in bfloat16 or wider, within the bound.
A program may use at most 128 MiB of HBM per device.

```python
import math
import jax
import jax.numpy as jnp
import numpy as np
from jax import lax

FC = 16384
FB = 65536
TC = 2048
TSUB = 64
SEG_DEV = 4
TOP = 2
CAP = 2
LC = 16
LF = 16
CSTRIDE = 2047
SUBBANKS = 16
SEGS = 128


def place_ends(values, rng, smallest, largest):
    spot = [jax.random.randint(jax.random.fold_in(rng, axis), (), 0, length) for axis, length in enumerate(values.shape)]
    main_axis = values.shape.index(max(values.shape))
    beside = spot[:main_axis] + [(spot[main_axis] + 1) % values.shape[main_axis]] + spot[main_axis + 1:]
    return values.at[tuple(spot)].set(smallest).at[tuple(beside)].set(largest)


def block_levels(stream_key, dims, shards, smallest, largest):
    loudness, own = 1.0, jax.random.fold_in(stream_key, 6)
    for position, parts in shards:
        steps = jnp.exp(jax.random.uniform(jax.random.fold_in(own, position), (parts,), jnp.float32, smallest / len(shards), largest / len(shards)))
        loudness = loudness * jnp.repeat(steps, dims[position] // parts).reshape([-1 if axis == position else 1 for axis in range(len(dims))])
    return loudness


def shared_out(stream_key, own, number, rows, count, top, reach, skew):
    ranking = jax.random.permutation(stream_key, count)
    packed, ordinary = portions_of(count, rows * top, reach, skew, True), portions_of(count, rows * top, reach, skew, False)
    places = jnp.arange(count)

    def named(lengths, rotation):
        used = int((lengths > 0).sum())
        fixed = max(1, used // 4)
        passed = fixed + (places - fixed + rotation * (used - fixed)) % max(1, count - fixed)
        return jnp.zeros((count,), jnp.int32).at[ranking[jnp.where(places < fixed, places, passed)]].set(jnp.asarray(lengths, jnp.int32))

    lengths = jnp.where(number % 4 == 0, named(packed, number // 4), named(ordinary, number - number // 4 - 1))
    mixed = jax.random.permutation(jax.random.fold_in(own, 3), count)
    source_of, sink = mixed[0:count // 2 * 2:2], mixed[1:count // 2 * 2:2]
    margin = jnp.minimum(lengths[source_of] - 1, reach - lengths[sink]) // 2
    margin = jnp.where((source_of == ranking[0]) | (sink == ranking[0]) | (lengths[sink] == 0), 0, jnp.maximum(margin, 0))
    passed = jax.random.randint(jax.random.fold_in(own, 4), (count // 2,), 0, 1 << 20) % (margin + 1)
    lengths = lengths.at[source_of].add(-passed).at[sink].add(passed)
    labels = jnp.searchsorted(jnp.cumsum(lengths), jnp.arange(rows * top), side="right").astype(jnp.int32)
    table = labels.reshape(top, rows).T
    table = table[jax.random.permutation(jax.random.fold_in(own, 1), rows)]
    rotation = jax.random.randint(jax.random.fold_in(own, 2), (rows, 1), 0, top)
    return jnp.take_along_axis(table, (jnp.arange(top)[None, :] + rotation) % top, axis=1)


def portions_of(amount, total, bound, skew, full):
    portions = [(1 << 20) // math.isqrt(standing ** skew) + 1 for standing in range(1, amount + 1)]
    largest = bound if full else min(bound, max(-(-total // amount), total * portions[0] // sum(portions)))
    least = 1 if total - largest >= amount - 1 else 0
    given, rest = [largest] + [least] * (amount - 1), total - largest - least * (amount - 1)
    while rest > 0:
        free = [i for i in range(1, amount) if given[i] < largest] or [i for i in range(1, amount) if given[i] < bound]
        pool, left = sum([portions[i] for i in free]), rest
        for i in free:
            addition = min(bound - given[i], max(1, left * portions[i] // pool), rest)
            given[i] = given[i] + addition
            rest = rest - addition
    return np.array(given)


def centred(rng, dims, width, limit, cuts=(), kind=jnp.bfloat16):
    array = width * jax.random.normal(rng, dims, jnp.float32)
    if cuts:
        array = array * block_levels(rng, dims, cuts, -0.22, 0.18)
    return jnp.clip(array, -limit, limit).astype(kind)


def setup_inputs(seed: int = 0, part: int = 0) -> dict:
    key_list = jax.random.split(jax.random.key(seed), 9)
    part_splits = jax.random.split(jax.random.fold_in(key_list[8], part), 9)
    coarse_spectra = centred(part_splits[0], (SEGS, 2, FC), 1.0, 6.0, ((0, 32), (2, 4)))
    fine_spectra = centred(part_splits[1], (SEGS, 2, FB), 1.0, 6.0, ((0, 32), (2, 4)))
    coarse_templates = centred(key_list[2], (2, TC, FC), 1.0, 6.0, ((1, 16), (2, 4)))
    fine_templates = centred(key_list[3], (2, SUBBANKS, TSUB, FB), 1.0, 6.0, ((1, 16), (3, 4)))
    coarse_weight = jnp.clip(jnp.exp(math.log(2.0) - 2.3025851 * jax.random.uniform(part_splits[4], (FC,), jnp.float32) ** block_levels(part_splits[4], (FC,), ((0, 4),), -0.2, 0.2)), 0.2, 2.0)
    fine_weight = jnp.clip(jnp.exp(math.log(2.0) - 2.3025851 * jax.random.uniform(part_splits[5], (FB,), jnp.float32) ** block_levels(part_splits[5], (FB,), ((0, 4),), -0.2, 0.2)), 0.2, 2.0)
    triggers_keys = jax.random.split(jax.random.fold_in(part_splits[6], 1), SEGS // SEG_DEV)
    triggers_turns = jax.random.permutation(jax.random.fold_in(part_splits[6], 3), SEGS // SEG_DEV)
    triggers = jax.vmap(lambda own, number: shared_out(jax.random.fold_in(part_splits[6], 2), own, number, SEG_DEV, SUBBANKS, TOP, CAP, 2))(triggers_keys, triggers_turns).reshape((SEGS, TOP))
    offsets = place_ends(jax.random.randint(part_splits[7], (SEGS, TOP), 0, 2 * FB - LF + 1), jax.random.fold_in(part_splits[7], 1), 0, 2 * FB - LF).astype(jnp.int32)
    return dict(coarse_spectra=coarse_spectra, fine_spectra=fine_spectra, coarse_templates=coarse_templates, fine_templates=fine_templates, coarse_weight=coarse_weight, fine_weight=fine_weight, triggers=triggers, offsets=offsets)


def phase_of(counts, period):
    radians = (2.0 * math.pi / period) * counts.astype(jnp.float32)
    return jnp.cos(radians), jnp.sin(radians)


def offset_count(freq_ids, offset, period):
    upper_bits = offset // 512
    lower_bits = offset % 512
    lower_term = (freq_ids * lower_bits) % period
    upper_term = ((freq_ids * upper_bits) % (period // 512)) * 512
    return (lower_term + upper_term) % period


def lagged(real_part, imag_part, lag_cos, lag_sin):
    left_real = real_part.T[:, :, None]
    left_imag = imag_part.T[:, :, None]
    right_cos = lag_cos[:, None, :]
    right_sin = lag_sin[:, None, :]
    lag_real = (left_real * right_cos - left_imag * right_sin).astype(jnp.bfloat16)
    lag_imag = (left_real * right_sin + left_imag * right_cos).astype(jnp.bfloat16)
    columns = real_part.shape[0] * lag_cos.shape[1]
    return lag_real.reshape(-1, columns), lag_imag.reshape(-1, columns)


def correlate(temp_real, temp_imag, lag_real, lag_imag):
    corr_real = jnp.dot(temp_real, lag_real, preferred_element_type=jnp.float32) + jnp.dot(temp_imag, lag_imag, preferred_element_type=jnp.float32)
    corr_imag = jnp.dot(temp_real, lag_imag, preferred_element_type=jnp.float32) - jnp.dot(temp_imag, lag_real, preferred_element_type=jnp.float32)
    return corr_real, corr_imag


def reference(coarse_spectra, fine_spectra, coarse_templates, fine_templates, coarse_weight, fine_weight, triggers, offsets):
    period_coarse = 2 * FC
    coarse_ids = jnp.arange(FC, dtype=jnp.int32)
    coarse_lags = jnp.arange(LC, dtype=jnp.int32) * CSTRIDE
    coarse_cos, coarse_sin = phase_of((coarse_ids[:, None] * coarse_lags[None, :]) % period_coarse, period_coarse)
    temp_real = coarse_templates[0]
    temp_imag = coarse_templates[1]
    coarse_norm = jnp.sum((temp_real.astype(jnp.float32) ** 2 + temp_imag.astype(jnp.float32) ** 2) * coarse_weight[None, :], axis=1)
    segment_blocks = coarse_spectra.reshape(SEGS // 8, 8, 2, FC)

    def coarse_block(segment_block):
        weighted = segment_block.astype(jnp.float32) * coarse_weight[None, None, :]
        lag_real, lag_imag = lagged(weighted[:, 0], weighted[:, 1], coarse_cos, coarse_sin)
        corr_real, corr_imag = correlate(temp_real, temp_imag, lag_real, lag_imag)
        energy = (corr_real * corr_real + corr_imag * corr_imag).reshape(TC, 8, LC)
        return jnp.max(energy, axis=2)

    peaks = lax.map(coarse_block, segment_blocks)
    coarse_snr = jnp.transpose(peaks, (1, 0, 2)).reshape(TC, SEGS) / coarse_norm[:, None]

    period_fine = 2 * FB
    fine_ids = jnp.arange(FB, dtype=jnp.int32)
    fine_lags = jnp.arange(LF, dtype=jnp.int32)
    fine_cos, fine_sin = phase_of((fine_ids[:, None] * fine_lags[None, :]) % period_fine, period_fine)
    fine_norm = jnp.sum((fine_templates[0].astype(jnp.float32) ** 2 + fine_templates[1].astype(jnp.float32) ** 2) * fine_weight[None, None, :], axis=2)
    pair_segments = jnp.repeat(jnp.arange(SEGS, dtype=jnp.int32), TOP)

    def fine_pair(pair):
        segment_id, bank_id, offset = pair
        spectrum = lax.dynamic_index_in_dim(fine_spectra, segment_id, 0, keepdims=False).astype(jnp.float32) * fine_weight[None, :]
        shift_cos, shift_sin = phase_of(offset_count(fine_ids, offset, period_fine), period_fine)
        shifted_real = spectrum[0] * shift_cos - spectrum[1] * shift_sin
        shifted_imag = spectrum[0] * shift_sin + spectrum[1] * shift_cos
        lag_real, lag_imag = lagged(shifted_real[None, :], shifted_imag[None, :], fine_cos, fine_sin)
        chosen = lax.dynamic_index_in_dim(fine_templates, bank_id, 1, keepdims=False)
        corr_real, corr_imag = correlate(chosen[0], chosen[1], lag_real, lag_imag)
        norm_row = lax.dynamic_index_in_dim(fine_norm, bank_id, 0, keepdims=False)
        return jnp.max(corr_real * corr_real + corr_imag * corr_imag, axis=1) / norm_row

    fine_rows = lax.map(fine_pair, (pair_segments, triggers.reshape(-1).astype(jnp.int32), offsets.reshape(-1).astype(jnp.int32)))
    return coarse_snr, fine_rows.reshape(SEGS, TOP, TSUB)
```

```python
import functools
import math

import jax
import jax.numpy as jnp
from jax import lax
from jax.experimental import pallas as pl
from jax.experimental.pallas import tpu as pltpu
from jax.sharding import PartitionSpec as P

FC = 16384
FB = 65536
CAP = 2
LC = 16
LF = 16
CSTRIDE = 2047
PERIOD = 131072
STEP = 512
LANES = 128
MESH = pl.DeviceIdType.MESH
NT = (((1,), (1,)), ((), ()))
NN = (((1,), (0,)), ((), ()))


def unit_phase(count):
    quadrant = (count + PERIOD // 8) >> 15
    x = (count - (quadrant << 15)).astype(jnp.float32) * (2.0 * math.pi / PERIOD)
    z = x * x
    s = x * (1.0 + z * (-1.0 / 6 + z * (1.0 / 120 + z * (-1.0 / 5040 + z * (1.0 / 362880)))))
    c = 1.0 + z * (-0.5 + z * (1.0 / 24 + z * (-1.0 / 720 + z * (1.0 / 40320 - z * (1.0 / 3628800)))))
    odd = (quadrant & 1) == 1
    cos = jnp.where(odd, s, c)
    sin = jnp.where(odd, c, s)
    cos = jnp.where(((quadrant + 1) & 2) == 2, -cos, cos)
    sin = jnp.where((quadrant & 2) == 2, -sin, sin)
    return cos, sin


def kernel(
    nb,
    nf,
    trig,
    offs,
    cs_hbm,
    fs_hbm,
    ct_hbm,
    ft_hbm,
    cw,
    fw,
    coarse_out,
    fine_out,
    cbuf,
    fbuf,
    ct,
    ft,
    ctab,
    ftab,
    clag,
    flag,
    cpq,
    fpq,
    sel,
    soff,
    cstage,
    crecv,
    fstage,
    frecv,
    nstage,
    nrecv,
    cnorm,
    fnorm,
    cres,
    rstage,
    rrecv,
    load_sem,
    ct_sem,
    ft_sem,
    c_send,
    c_recv,
    f_send,
    f_recv,
    n_send,
    n_recv,
    cx_send,
    cx_recv,
    fx_send,
    fx_recv,
    r_send,
    r_recv,
):
    me = lax.axis_index("bank")
    fx = lax.axis_index("freq")
    groups = nb // 4
    segs = cbuf.shape[1] // 2
    cbins = cbuf.shape[2]
    fbins = fbuf.shape[2]
    parts = f_send.shape[1]
    fpart = fbins // parts
    ctn = ct.shape[0] // 2
    ftn = ft.shape[0] // 2
    cq = ctn // nf
    fq = ftn // nf
    scale = PERIOD // (2 * FC)

    def source(p):
        step = (nb - (p + 1) // 2) if p % 2 else p // 2
        return lax.rem(me + step, nb)

    def other(k):
        return lax.rem(fx + k, nf)

    right = lax.rem(me + 1, nb)
    left = lax.rem(me + nb - 1, nb)

    def c_move(p):
        return pltpu.make_async_remote_copy(
            src_ref=cbuf.at[max(p - 2, 0)],
            dst_ref=cbuf.at[p],
            send_sem=c_send.at[p],
            recv_sem=c_recv.at[p],
            device_id={"bank": right if p % 2 else left},
            device_id_type=MESH,
        )

    def f_move(p, c):
        last = p == nb - 1
        leftward = p % 2 == 0 or (last and c >= parts // 2)
        origin = p - 1 if (last and leftward) else max(p - 2, 0)
        part = pl.ds(c * fpart, fpart)
        return pltpu.make_async_remote_copy(
            src_ref=fbuf.at[origin, :, part],
            dst_ref=fbuf.at[p, :, part],
            send_sem=f_send.at[p, c],
            recv_sem=f_recv.at[p, c],
            device_id={"bank": left if leftward else right},
            device_id_type=MESH,
        )

    def n_move(k):
        return pltpu.make_async_remote_copy(
            src_ref=nstage.at[other(k)],
            dst_ref=nrecv.at[k - 1],
            send_sem=n_send.at[k - 1],
            recv_sem=n_recv.at[k - 1],
            device_id={"freq": other(k)},
            device_id_type=MESH,
        )

    def cx_move(g, k):
        return pltpu.make_async_remote_copy(
            src_ref=cstage.at[g, other(k)],
            dst_ref=crecv.at[g, k - 1],
            send_sem=cx_send.at[g, k - 1],
            recv_sem=cx_recv.at[g, k - 1],
            device_id={"freq": other(k)},
            device_id_type=MESH,
        )

    def fx_move(g, k):
        return pltpu.make_async_remote_copy(
            src_ref=fstage.at[g, other(k)],
            dst_ref=frecv.at[g, k - 1],
            send_sem=fx_send.at[g, k - 1],
            recv_sem=fx_recv.at[g, k - 1],
            device_id={"freq": other(k)},
            device_id_type=MESH,
        )

    def r_move(p):
        return pltpu.make_async_remote_copy(
            src_ref=rstage.at[p // 4],
            dst_ref=rrecv.at[p],
            send_sem=r_send.at[p],
            recv_sem=r_recv.at[p],
            device_id={"bank": source(p)},
            device_id_type=MESH,
        )

    own_c = pltpu.make_async_copy(cs_hbm, cbuf.at[0], load_sem.at[0])
    own_f = pltpu.make_async_copy(fs_hbm, fbuf.at[0], load_sem.at[1])
    own_c.start()
    own_f.start()
    load_ct = pltpu.make_async_copy(ct_hbm, ct, ct_sem)
    load_ft = pltpu.make_async_copy(ft_hbm, ft, ft_sem)
    load_ct.start()
    load_ft.start()

    barrier = pltpu.get_barrier_semaphore()
    for neighbour in (left, right):
        pl.semaphore_signal(barrier, inc=1, device_id={"bank": neighbour}, device_id_type=MESH)
    for k in range(1, nf):
        pl.semaphore_signal(barrier, inc=1, device_id={"freq": other(k)}, device_id_type=MESH)
    own_c.wait()
    own_f.wait()
    pl.semaphore_wait(barrier, 2 + nf - 1)

    for p in (1, 2):
        c_move(p).start()
    for c in range(parts):
        for p in (1, 2):
            f_move(p, c).start()

    def c_phases(i, carry):
        at = pl.ds(pl.multiple_of(i * STEP, STEP), STEP)
        lag = lax.broadcasted_iota(jnp.int32, (LC, STEP), 0) * CSTRIDE
        f = fx * cbins + i * STEP + lax.broadcasted_iota(jnp.int32, (LC, STEP), 1)
        cos, sin = unit_phase((f * lag * scale) & (PERIOD - 1))
        w = cw[:, at]
        ctab[0, :, at] = cos * w
        ctab[1, :, at] = sin * w
        return carry

    lax.fori_loop(0, cbins // STEP, c_phases, 0)

    def f_phases(i, carry):
        at = pl.ds(pl.multiple_of(i * STEP, STEP), STEP)
        lag = lax.broadcasted_iota(jnp.int32, (LF, STEP), 0)
        f = fx * fbins + i * STEP + lax.broadcasted_iota(jnp.int32, (LF, STEP), 1)
        cos, sin = unit_phase((f * lag) & (PERIOD - 1))
        w = fw[:, at]
        ftab[0, :, at] = cos * w
        ftab[1, :, at] = sin * w
        return carry

    lax.fori_loop(0, fbins // STEP, f_phases, 0)

    rows = lax.broadcasted_iota(jnp.int32, (16, 8 * segs), 0)
    cols = lax.broadcasted_iota(jnp.int32, (16, 8 * segs), 1)
    orow = lax.broadcasted_iota(jnp.int32, (8, LANES), 0)
    for g in range(groups):
        pick = jnp.zeros((16, 8 * segs), jnp.float32)
        shift = jnp.zeros((8, LANES), jnp.int32)
        for i in range(4):
            base = source(4 * g + i) * segs
            found = jnp.int32(0)
            for s in range(segs):
                for k in range(2):
                    hit = jnp.where(trig[base + s, k] == me, 1, 0)
                    slot = 2 * i + found
                    col = (i * segs + s) * 2
                    here = ((rows == slot) & (cols == col)) | ((rows == 8 + slot) & (cols == col + 1))
                    pick += jnp.where(here, hit.astype(jnp.float32), 0.0)
                    shift += jnp.where(orow == slot, hit * offs[base + s, k], 0)
                    found = found + hit
        sel[g] = pick.astype(jnp.bfloat16)
        soff[g] = shift

    load_ct.wait()

    def c_power(i, total):
        at = pl.ds(pl.multiple_of(i * LANES, LANES), LANES)
        re = ct[:ctn, at].astype(jnp.float32)
        im = ct[ctn:, at].astype(jnp.float32)
        return total + (re * re + im * im) * cw[:, at]

    ct_sum = lax.fori_loop(0, cbins // LANES, c_power, jnp.zeros((ctn, LANES), jnp.float32))
    ct_sum = jnp.broadcast_to(jnp.sum(ct_sum, axis=1, keepdims=True), (ctn, LANES))
    load_ft.wait()

    def f_power(i, total):
        at = pl.ds(pl.multiple_of(i * LANES, LANES), LANES)
        re = ft[:ftn, at].astype(jnp.float32)
        im = ft[ftn:, at].astype(jnp.float32)
        return total + (re * re + im * im) * fw[:, at]

    ft_sum = lax.fori_loop(0, fbins // LANES, f_power, jnp.zeros((ftn, LANES), jnp.float32))
    ft_sum = jnp.broadcast_to(jnp.sum(ft_sum, axis=1, keepdims=True), (ftn, LANES))
    for q in range(nf):
        nstage[q, :cq] = ct_sum[q * cq : (q + 1) * cq]
        nstage[q, cq:] = ft_sum[q * fq : (q + 1) * fq]

    def coarse_group(g):
        prow = lax.broadcasted_iota(jnp.int32, (8 * segs, 8 * segs), 0)
        pcol = lax.broadcasted_iota(jnp.int32, (8 * segs, 8 * segs), 1)
        half = 4 * segs
        want = jnp.where(prow < half, 2 * prow, 2 * (prow - half) + 1)
        split = jnp.where(pcol == want, 1.0, 0.0).astype(jnp.bfloat16)
        cpq[...] = jnp.zeros_like(cpq)
        ncol = LC * half

        def step(i, carry):
            at = pl.ds(pl.multiple_of(i * STEP, STEP), STEP)
            block = jnp.concatenate([cbuf[4 * g + b, :, at].astype(jnp.float32) for b in range(4)], axis=0)
            y = lax.dot_general(split, block.astype(jnp.bfloat16), NN, preferred_element_type=jnp.float32)
            yr, yi = y[:half], y[half:]
            for j in range(LC):
                c = ctab[0, j : j + 1, at]
                s = ctab[1, j : j + 1, at]
                clag[j * half : (j + 1) * half] = (yr * c - yi * s).astype(jnp.bfloat16)
                clag[ncol + j * half : ncol + (j + 1) * half] = (yr * s + yi * c).astype(jnp.bfloat16)
            cpq[...] += lax.dot_general(ct[:, at], clag[...], NT, preferred_element_type=jnp.float32)
            return carry

        lax.fori_loop(0, cbins // STEP, step, 0)
        re = cpq[:ctn, :ncol] + cpq[ctn:, ncol:]
        im = cpq[:ctn, ncol:] - cpq[ctn:, :ncol]
        for q in range(nf):
            cstage[g, q, :cq] = re[q * cq : (q + 1) * cq]
            cstage[g, q, cq:] = im[q * cq : (q + 1) * cq]

    def fine_piece(g, c):
        ncol = LF * 8
        if c == 0:
            fpq[...] = jnp.zeros_like(fpq)

        def step(i, carry):
            begin = c * fpart + i * STEP
            at = pl.ds(pl.multiple_of(begin, STEP), STEP)
            block = jnp.concatenate([fbuf[4 * g + b, :, at].astype(jnp.float32) for b in range(4)], axis=0)
            y = lax.dot_general(sel[g], block.astype(jnp.bfloat16), NN, preferred_element_type=jnp.float32)
            yr, yi = y[:8], y[8:]
            f = fx * fbins + begin + lax.broadcasted_iota(jnp.int32, (8, STEP), 1)
            cos, sin = unit_phase((f * soff[g, :, 0:1]) & (PERIOD - 1))
            sr = yr * cos - yi * sin
            si = yr * sin + yi * cos
            for j in range(0, LF, 2):
                res, ims = [], []
                for jj in (j, j + 1):
                    wc = ftab[0, jj : jj + 1, at]
                    ws = ftab[1, jj : jj + 1, at]
                    res.append(sr * wc - si * ws)
                    ims.append(sr * ws + si * wc)
                flag[j * 8 : j * 8 + 16] = jnp.concatenate(res, axis=0).astype(jnp.bfloat16)
                flag[ncol + j * 8 : ncol + j * 8 + 16] = jnp.concatenate(ims, axis=0).astype(jnp.bfloat16)
            fpq[...] += lax.dot_general(ft[:, at], flag[...], NT, preferred_element_type=jnp.float32)
            return carry

        lax.fori_loop(0, fpart // STEP, step, 0)
        if c == parts - 1:
            re = fpq[:ftn, :ncol] + fpq[ftn:, ncol:]
            im = fpq[:ftn, ncol:] - fpq[ftn:, :ncol]
            for q in range(nf):
                fstage[g, q, :fq] = re[q * fq : (q + 1) * fq]
                fstage[g, q, fq:] = im[q * fq : (q + 1) * fq]

    def coarse_peak(g):
        total = cstage[g, fx]
        for k in range(1, nf):
            cx_move(g, k).wait_recv()
            total = total + crecv[g, k - 1]
        energy = total[:cq] * total[:cq] + total[cq:] * total[cq:]
        half = 4 * segs
        peak = energy[:, :LANES]
        for b in range(1, LC * half // LANES):
            peak = jnp.maximum(peak, energy[:, b * LANES : (b + 1) * LANES])
        span = LANES // 2
        while span >= half:
            peak = jnp.maximum(peak, pltpu.roll(peak, span, 1))
            span //= 2
        peak = peak / cnorm[...]
        lane = lax.broadcasted_iota(jnp.int32, (cq, LANES), 1) // segs
        for i in range(4):
            src = source(4 * g + i)
            moved = pltpu.roll(peak, lax.rem(src * segs + LANES - i * segs, LANES), 1)
            cres[...] = jnp.where(lane == src, moved, cres[...])

    def fine_peak(g):
        total = fstage[g, fx]
        for k in range(1, nf):
            fx_move(g, k).wait_recv()
            total = total + frecv[g, k - 1]
        energy = total[:fq] * total[:fq] + total[fq:] * total[fq:]
        peak = energy
        span = LANES // 2
        while span >= 8:
            peak = jnp.maximum(peak, pltpu.roll(peak, span, 1))
            span //= 2
        peak = peak / fnorm[...]
        square = jnp.concatenate([peak, jnp.zeros((LANES - fq, LANES), jnp.float32)], axis=0)
        rstage[g] = square.T[:8]

    def norms():
        total = nstage[fx]
        for k in range(1, nf):
            n_move(k).wait_recv()
            total = total + nrecv[k - 1]
        cnorm[...] = total[:cq]
        fnorm[...] = total[cq:]
        cres[...] = jnp.zeros_like(cres)

    def give_back(g):
        for p in range(4 * g, 4 * g + 4):
            if p > 0:
                r_move(p).start()

    for g in range(groups):
        for h in (2 * g + 1, 2 * g + 2):
            second = h == 2 * g + 2
            here = [p for p in (2 * h - 1, 2 * h) if p <= nb - 1]
            for p in here:
                c_move(p).wait_recv()
                if p + 2 <= nb - 1:
                    c_move(p + 2).start()
            if second:
                coarse_group(g)
            order = list(range(parts))
            if here == [nb - 1]:
                order = [c for pair in zip(order[: parts // 2], order[parts // 2 :]) for c in pair]
            for c in order:
                for p in here:
                    f_move(p, c).wait_recv()
                    if p + 2 <= nb - 1 and not (p + 2 == nb - 1 and c >= parts // 2):
                        f_move(p + 2, c).start()
                    if p + 1 == nb - 1 and c >= parts // 2:
                        f_move(p + 1, c).start()
                if second:
                    fine_piece(g, c)
                    if c == 0:
                        for k in range(1, nf):
                            cx_move(g, k).start()
                elif g == 0 and c == 0:
                    for k in range(1, nf):
                        n_move(k).start()
            if not second and g == 0:
                norms()
            if not second and g > 0:
                coarse_peak(g - 1)
                fine_peak(g - 1)
                give_back(g - 1)
        for k in range(1, nf):
            fx_move(g, k).start()
    coarse_peak(groups - 1)
    fine_peak(groups - 1)
    give_back(groups - 1)
    coarse_out[...] = cres[...]
    rrecv[0] = rstage[0]
    for p in range(1, nb):
        r_move(p).wait_recv()

    result = jnp.zeros((8, LANES), jnp.float32)
    named = []
    for s in range(segs):
        for k in range(2):
            bank = trig[me * segs + s, k]
            rank = jnp.int32(0)
            for before in named:
                rank = rank + jnp.where(before == bank, 1, 0)
            named.append(bank)
            away = lax.rem(me - bank + nb, nb)
            place = jnp.where(away < nb // 2, 2 * away, 2 * (nb - away) - 1)
            row = lax.rem(place, 4) * 2 + rank
            tile = rrecv[place]
            line = jnp.sum(jnp.where(orow == row, tile, 0.0), axis=0, keepdims=True)
            result = jnp.where(orow == 2 * s + k, line, result)
    fine_out[...] = result

    for p in range(1, nb):
        c_move(p).wait_send()
        for c in range(parts):
            f_move(p, c).wait_send()
        r_move(p).wait_send()
    for k in range(1, nf):
        n_move(k).wait_send()
        for g in range(groups):
            cx_move(g, k).wait_send()
            fx_move(g, k).wait_send()


def body(
    nb,
    nf,
    coarse_spectra,
    fine_spectra,
    coarse_templates,
    fine_templates,
    coarse_weight,
    fine_weight,
    triggers,
    offsets,
):
    segs, _, cbins = coarse_spectra.shape
    fbins = fine_spectra.shape[2]
    ctn = coarse_templates.shape[1]
    ftn = fine_templates.shape[2]
    groups = nb // 4
    parts = 4
    cq, fq = ctn // nf, ftn // nf
    ccol, fcol = LC * 4 * segs, LF * 8
    f32, bf16 = jnp.float32, jnp.bfloat16
    dma = pltpu.SemaphoreType.DMA
    anywhere = pl.BlockSpec(memory_space=pl.ANY)
    smem = pl.BlockSpec(memory_space=pltpu.SMEM)
    vmem = pl.BlockSpec(memory_space=pltpu.VMEM)
    coarse, fine = pl.pallas_call(
        functools.partial(kernel, nb, nf),
        out_shape=(
            jax.ShapeDtypeStruct((cq, LANES), f32),
            jax.ShapeDtypeStruct((8, LANES), f32),
        ),
        in_specs=[smem, smem, anywhere, anywhere, anywhere, anywhere, vmem, vmem],
        out_specs=(vmem, vmem),
        scratch_shapes=[
            pltpu.VMEM((nb, 2 * segs, cbins), bf16),
            pltpu.VMEM((nb, 2 * segs, fbins), bf16),
            pltpu.VMEM((2 * ctn, cbins), bf16),
            pltpu.VMEM((2 * ftn, fbins), bf16),
            pltpu.VMEM((2, LC, cbins), f32),
            pltpu.VMEM((2, LF, fbins), f32),
            pltpu.VMEM((2 * ccol, STEP), bf16),
            pltpu.VMEM((2 * fcol, STEP), bf16),
            pltpu.VMEM((2 * ctn, 2 * ccol), f32),
            pltpu.VMEM((2 * ftn, 2 * fcol), f32),
            pltpu.VMEM((groups, 16, 8 * segs), bf16),
            pltpu.VMEM((groups, 8, LANES), jnp.int32),
            pltpu.VMEM((groups, nf, 2 * cq, ccol), f32),
            pltpu.VMEM((groups, nf - 1, 2 * cq, ccol), f32),
            pltpu.VMEM((groups, nf, 2 * fq, fcol), f32),
            pltpu.VMEM((groups, nf - 1, 2 * fq, fcol), f32),
            pltpu.VMEM((nf, cq + fq, LANES), f32),
            pltpu.VMEM((nf - 1, cq + fq, LANES), f32),
            pltpu.VMEM((cq, LANES), f32),
            pltpu.VMEM((fq, LANES), f32),
            pltpu.VMEM((cq, LANES), f32),
            pltpu.VMEM((groups, 8, LANES), f32),
            pltpu.VMEM((nb, 8, LANES), f32),
            dma((2,)),
            dma,
            dma,
            dma((nb,)),
            dma((nb,)),
            dma((nb, parts)),
            dma((nb, parts)),
            dma((nf - 1,)),
            dma((nf - 1,)),
            dma((groups, nf - 1)),
            dma((groups, nf - 1)),
            dma((groups, nf - 1)),
            dma((groups, nf - 1)),
            dma((nb,)),
            dma((nb,)),
        ],
        compiler_params=pltpu.CompilerParams(
            collective_id=0, has_side_effects=True, vmem_limit_bytes=48 * 1024 * 1024
        ),
        name="search",
    )(
        triggers,
        offsets,
        coarse_spectra.reshape(2 * segs, cbins),
        fine_spectra.reshape(2 * segs, fbins),
        coarse_templates.reshape(2 * ctn, cbins),
        fine_templates.reshape(2 * ftn, fbins),
        coarse_weight.reshape(1, cbins),
        fine_weight.reshape(1, fbins),
    )
    coarse_snr = coarse[:, : nb * segs]
    fine_snr = fine[:, :fq].reshape(segs, 2, fq)
    return coarse_snr, fine_snr


def solution(mesh):
    return jax.shard_map(
        functools.partial(body, mesh.shape["bank"], mesh.shape["freq"]),
        mesh=mesh,
        in_specs=(
            P(("groups", "seg", "bank"), None, "freq"),
            P(("groups", "seg", "bank"), None, "freq"),
            P(None, "bank", "freq"),
            P(None, "bank", None, "freq"),
            P(("groups", "freq")),
            P(("groups", "freq")),
            P(("groups", "seg"), None),
            P(("groups", "seg"), None),
        ),
        out_specs=(
            P(("bank", "freq"), ("groups", "seg")),
            P(("groups", "seg", "bank"), None, "freq"),
        ),
        check_vma=False,
    )
```

```python
import functools
import math

import jax
import jax.numpy as jnp
from jax import lax
from jax.experimental import pallas as pl
from jax.experimental.pallas import tpu as pltpu
from jax.sharding import PartitionSpec as P

FC = 16384
FB = 65536
CAP = 2
LC = 16
LF = 16
CSTRIDE = 2047
PERIOD = 131072
STEP = 512
DEEP = 2048
LANES = 128
MESH = pl.DeviceIdType.MESH
NT = (((1,), (1,)), ((), ()))
NN = (((1,), (0,)), ((), ()))


def unit_phase(count):
    quadrant = (count + PERIOD // 8) >> 15
    x = (count - (quadrant << 15)).astype(jnp.float32) * (2.0 * math.pi / PERIOD)
    z = x * x
    s = x * (1.0 + z * (-1.0 / 6 + z * (1.0 / 120 + z * (-1.0 / 5040 + z * (1.0 / 362880)))))
    c = 1.0 + z * (-0.5 + z * (1.0 / 24 + z * (-1.0 / 720 + z * (1.0 / 40320 - z * (1.0 / 3628800)))))
    odd = (quadrant & 1) == 1
    cos = jnp.where(odd, s, c)
    sin = jnp.where(odd, c, s)
    cos = jnp.where(((quadrant + 1) & 2) == 2, -cos, cos)
    sin = jnp.where((quadrant & 2) == 2, -sin, sin)
    return cos, sin


def kernel(
    nb,
    nf,
    trig,
    offs,
    cs_hbm,
    fs_hbm,
    ct_hbm,
    ft_hbm,
    cw_hbm,
    fw_hbm,
    coarse_out,
    fine_out,
    craw,
    fraw,
    cbuf,
    fbuf,
    ct,
    ft,
    cw,
    fw,
    cpure,
    fpure,
    ctab,
    ftab,
    clag,
    flag,
    cpq,
    fpq,
    sel,
    soff,
    cstage,
    crecv,
    fstage,
    frecv,
    nstage,
    nrecv,
    cnorm,
    fnorm,
    cres,
    rstage,
    rrecv,
    load_sem,
    w_sem,
    ct_sem,
    ft_sem,
    c_send,
    c_recv,
    f_send,
    f_recv,
    n_send,
    n_recv,
    cx_send,
    cx_recv,
    fx_send,
    fx_recv,
    r_send,
    r_recv,
):
    me = lax.axis_index("bank")
    fx = lax.axis_index("freq")
    groups = nb // 4
    segs = cbuf.shape[1] // 2
    cbins = cbuf.shape[2]
    fbins = fbuf.shape[2]
    parts = f_send.shape[1]
    fpart = fbins // parts
    ctn = ct.shape[0] // 2
    ftn = ft.shape[0] // 2
    cq = ctn // nf
    fq = ftn // nf
    scale = PERIOD // (2 * FC)

    def source(p):
        step = (nb - (p + 1) // 2) if p % 2 else p // 2
        return lax.rem(me + step, nb)

    def other(k):
        return lax.rem(fx + k, nf)

    right = lax.rem(me + 1, nb)
    left = lax.rem(me + nb - 1, nb)

    def c_move(p):
        return pltpu.make_async_remote_copy(
            src_ref=cbuf.at[max(p - 2, 0)],
            dst_ref=cbuf.at[p],
            send_sem=c_send.at[p],
            recv_sem=c_recv.at[p],
            device_id={"bank": right if p % 2 else left},
            device_id_type=MESH,
        )

    def f_move(p, c):
        last = p == nb - 1
        leftward = p % 2 == 0 or (last and not isinstance(c, jax.Array) and c >= parts // 2)
        origin = p - 1 if (last and leftward) else max(p - 2, 0)
        part = pl.ds(pl.multiple_of(c * fpart, fpart), fpart)
        return pltpu.make_async_remote_copy(
            src_ref=fbuf.at[origin, :, part],
            dst_ref=fbuf.at[p, :, part],
            send_sem=f_send.at[p, c],
            recv_sem=f_recv.at[p, c],
            device_id={"bank": left if leftward else right},
            device_id_type=MESH,
        )

    def n_move(k):
        return pltpu.make_async_remote_copy(
            src_ref=nstage.at[other(k)],
            dst_ref=nrecv.at[k - 1],
            send_sem=n_send.at[k - 1],
            recv_sem=n_recv.at[k - 1],
            device_id={"freq": other(k)},
            device_id_type=MESH,
        )

    def cx_move(g, k):
        return pltpu.make_async_remote_copy(
            src_ref=cstage.at[g, other(k)],
            dst_ref=crecv.at[g, k - 1],
            send_sem=cx_send.at[g, k - 1],
            recv_sem=cx_recv.at[g, k - 1],
            device_id={"freq": other(k)},
            device_id_type=MESH,
        )

    def fx_move(g, k):
        return pltpu.make_async_remote_copy(
            src_ref=fstage.at[g, other(k)],
            dst_ref=frecv.at[g, k - 1],
            send_sem=fx_send.at[g, k - 1],
            recv_sem=fx_recv.at[g, k - 1],
            device_id={"freq": other(k)},
            device_id_type=MESH,
        )

    def r_move(p):
        return pltpu.make_async_remote_copy(
            src_ref=rstage.at[p // 4],
            dst_ref=rrecv.at[p],
            send_sem=r_send.at[p],
            recv_sem=r_recv.at[p],
            device_id={"bank": source(p)},
            device_id_type=MESH,
        )

    own_c = pltpu.make_async_copy(cs_hbm, craw, load_sem.at[0])
    own_f = pltpu.make_async_copy(fs_hbm, fraw, load_sem.at[1])
    own_c.start()
    own_f.start()
    load_cw = pltpu.make_async_copy(cw_hbm, cw, w_sem.at[0])
    load_fw = pltpu.make_async_copy(fw_hbm, fw, w_sem.at[1])
    load_cw.start()
    load_fw.start()
    load_ct = pltpu.make_async_copy(ct_hbm, ct, ct_sem)
    load_ft = pltpu.make_async_copy(ft_hbm, ft, ft_sem)
    load_ct.start()
    load_ft.start()

    barrier = pltpu.get_barrier_semaphore()
    for neighbour in (left, right):
        pl.semaphore_signal(barrier, inc=1, device_id={"bank": neighbour}, device_id_type=MESH)
    for k in range(1, nf):
        pl.semaphore_signal(barrier, inc=1, device_id={"freq": other(k)}, device_id_type=MESH)
    own_c.wait()
    own_f.wait()

    def settle(raw, buf, begin, size):
        for at in range(begin, begin + size, STEP):
            piece = [raw[r, :, at : at + STEP].astype(jnp.float32) for r in range(segs)]
            buf[0, :, at : at + STEP] = jnp.concatenate(piece, axis=0).astype(jnp.bfloat16)

    settle(craw, cbuf, 0, cbins)
    settle(fraw, fbuf, 0, fpart)
    pl.semaphore_wait(barrier, 2 + nf - 1)
    for p in (1, 2):
        c_move(p).start()
    for c in range(parts):
        if c + 1 < parts:
            settle(fraw, fbuf, (c + 1) * fpart, fpart)
        for p in (1, 2):
            f_move(p, c).start()
    load_cw.wait()
    load_fw.wait()

    def c_phases(i, carry):
        at = pl.ds(pl.multiple_of(i * STEP, STEP), STEP)
        lag = lax.broadcasted_iota(jnp.int32, (LC, STEP), 0) * CSTRIDE
        f = fx * cbins + i * STEP + lax.broadcasted_iota(jnp.int32, (LC, STEP), 1)
        cos, sin = unit_phase((f * lag * scale) & (PERIOD - 1))
        w = cw[:, at]
        ctab[0, :, at] = cos * w
        ctab[1, :, at] = sin * w
        return carry

    lax.fori_loop(0, cbins // STEP, c_phases, 0)

    def f_phases(i, carry):
        at = pl.ds(pl.multiple_of(i * STEP, STEP), STEP)
        lag = lax.broadcasted_iota(jnp.int32, (LF, STEP), 0)
        f = fx * fbins + i * STEP + lax.broadcasted_iota(jnp.int32, (LF, STEP), 1)
        cos, sin = unit_phase((f * lag) & (PERIOD - 1))
        w = fw[:, at]
        ftab[0, :, at] = cos * w
        ftab[1, :, at] = sin * w
        return carry

    lax.fori_loop(0, fbins // STEP, f_phases, 0)

    rows = lax.broadcasted_iota(jnp.int32, (16, 8 * segs), 0)
    cols = lax.broadcasted_iota(jnp.int32, (16, 8 * segs), 1)
    orow = lax.broadcasted_iota(jnp.int32, (8, LANES), 0)
    for g in range(groups):
        pick = jnp.zeros((16, 8 * segs), jnp.float32)
        shift = jnp.zeros((8, LANES), jnp.int32)
        for i in range(4):
            base = source(4 * g + i) * segs
            found = jnp.int32(0)
            for s in range(segs):
                for k in range(2):
                    hit = jnp.where(trig[k, base + s] == me, 1, 0)
                    slot = 2 * i + found
                    col = (i * segs + s) * 2
                    here = ((rows == slot) & (cols == col)) | ((rows == 8 + slot) & (cols == col + 1))
                    pick += jnp.where(here, hit.astype(jnp.float32), 0.0)
                    shift += jnp.where(orow == slot, hit * offs[k, base + s], 0)
                    found = found + hit
        sel[g] = pick.astype(jnp.bfloat16)
        soff[g] = shift

    def powers():
        load_ct.wait()

        def c_power(i, total):
            at = pl.ds(pl.multiple_of(i * LANES, LANES), LANES)
            re = ct[:ctn, at].astype(jnp.float32)
            im = ct[ctn:, at].astype(jnp.float32)
            return total + (re * re + im * im) * cw[:, at]

        ct_sum = lax.fori_loop(0, cbins // LANES, c_power, jnp.zeros((ctn, LANES), jnp.float32))
        ct_sum = jnp.broadcast_to(jnp.sum(ct_sum, axis=1, keepdims=True), (ctn, LANES))
        load_ft.wait()

        def f_power(i, total):
            at = pl.ds(pl.multiple_of(i * LANES, LANES), LANES)
            re = ft[:ftn, at].astype(jnp.float32)
            im = ft[ftn:, at].astype(jnp.float32)
            return total + (re * re + im * im) * fw[:, at]

        ft_sum = lax.fori_loop(0, fbins // LANES, f_power, jnp.zeros((ftn, LANES), jnp.float32))
        ft_sum = jnp.broadcast_to(jnp.sum(ft_sum, axis=1, keepdims=True), (ftn, LANES))
        for q in range(nf):
            nstage[q, :cq] = ct_sum[q * cq : (q + 1) * cq]
            nstage[q, cq:] = ft_sum[q * fq : (q + 1) * fq]

    def coarse_group(g):
        half = 4 * segs
        prow = lax.broadcasted_iota(jnp.int32, (2 * half, 2 * half), 0)
        pcol = lax.broadcasted_iota(jnp.int32, (2 * half, 2 * half), 1)
        want = jnp.where(prow < half, 2 * prow, 2 * (prow - half) + 1)
        split = jnp.where(pcol == want, 1.0, 0.0).astype(jnp.bfloat16)
        ncol = LC * half
        wide = min(2 * STEP, cbins)
        for begin in range(0, cbins, wide):
            at = slice(begin, begin + wide)
            block = jnp.concatenate([cbuf[4 * g + b, :, at].astype(jnp.float32) for b in range(4)], axis=0)
            cpure[:, at] = lax.dot_general(split, block.astype(jnp.bfloat16), NN, preferred_element_type=jnp.float32)
        cpq[...] = jnp.zeros_like(cpq)
        deep = min(DEEP, cbins)

        def step(i, carry):
            base = pl.multiple_of(i * deep, deep)
            for kt in range(0, deep, 2 * LANES):
                at = pl.ds(base + kt, 2 * LANES)
                yr, yi = cpure[:half, at], cpure[half:, at]
                for j in range(LC):
                    c = ctab[0, j : j + 1, at]
                    s = ctab[1, j : j + 1, at]
                    clag[j * half : (j + 1) * half, kt : kt + 2 * LANES] = (yr * c - yi * s).astype(jnp.bfloat16)
                    clag[ncol + j * half : ncol + (j + 1) * half, kt : kt + 2 * LANES] = (yr * s + yi * c).astype(jnp.bfloat16)
            cpq[...] += lax.dot_general(clag[...], ct[:, pl.ds(base, deep)], NT, preferred_element_type=jnp.float32)
            return carry

        lax.fori_loop(0, cbins // deep, step, 0)
        re = (cpq[:ncol, :ctn] + cpq[ncol:, ctn:]).T
        im = (cpq[ncol:, :ctn] - cpq[:ncol, ctn:]).T
        for q in range(nf):
            cstage[g, q, :cq] = re[q * cq : (q + 1) * cq]
            cstage[g, q, cq:] = im[q * cq : (q + 1) * cq]

    def fine_piece(g, c):
        ncol = LF * 8
        wide = min(2 * STEP, fpart)
        for begin in range(0, fpart, wide):
            first = c * fpart + begin
            at = pl.ds(pl.multiple_of(first, wide), wide)
            block = jnp.concatenate([fbuf[4 * g + b, :, at].astype(jnp.float32) for b in range(4)], axis=0)
            y = lax.dot_general(sel[g], block.astype(jnp.bfloat16), NN, preferred_element_type=jnp.float32)
            f = fx * fbins + first + lax.broadcasted_iota(jnp.int32, (8, wide), 1)
            shift = jnp.concatenate([soff[g]] * (wide // LANES), axis=1)
            cos, sin = unit_phase((f * shift) & (PERIOD - 1))
            yr, yi = y[:8], y[8:]
            fpure[:8, begin : begin + wide] = yr * cos - yi * sin
            fpure[8:, begin : begin + wide] = yr * sin + yi * cos
        deep = min(DEEP, fpart)

        def step(i, carry):
            base = pl.multiple_of(i * deep, deep)
            whole = pl.multiple_of(c * fpart + i * deep, deep)
            for kt in range(0, deep, 2 * LANES):
                sr = fpure[:8, pl.ds(base + kt, 2 * LANES)]
                si = fpure[8:, pl.ds(base + kt, 2 * LANES)]
                at = pl.ds(whole + kt, 2 * LANES)
                for j in range(0, LF, 2):
                    res, ims = [], []
                    for jj in (j, j + 1):
                        wc = ftab[0, jj : jj + 1, at]
                        ws = ftab[1, jj : jj + 1, at]
                        res.append(sr * wc - si * ws)
                        ims.append(sr * ws + si * wc)
                    here = slice(kt, kt + 2 * LANES)
                    flag[j * 8 : j * 8 + 16, here] = jnp.concatenate(res, axis=0).astype(jnp.bfloat16)
                    flag[ncol + j * 8 : ncol + j * 8 + 16, here] = jnp.concatenate(ims, axis=0).astype(jnp.bfloat16)
            fpq[...] += lax.dot_general(flag[...], ft[:, pl.ds(whole, deep)], NT, preferred_element_type=jnp.float32)
            return carry

        lax.fori_loop(0, fpart // deep, step, 0)

    def fine_done(g):
        ncol = LF * 8
        top, bottom = fpq[:ncol], fpq[ncol:]
        re = (top + pltpu.roll(bottom, ftn, 1)).T
        im = (bottom - pltpu.roll(top, ftn, 1)).T
        for q in range(nf):
            fstage[g, q, :fq] = re[q * fq : (q + 1) * fq]
            fstage[g, q, fq:] = im[q * fq : (q + 1) * fq]

    def coarse_peak(g):
        total = cstage[g, fx]
        for k in range(1, nf):
            cx_move(g, k).wait_recv()
            total = total + crecv[g, k - 1]
        energy = total[:cq] * total[:cq] + total[cq:] * total[cq:]
        half = 4 * segs
        peak = energy[:, :LANES]
        for b in range(1, LC * half // LANES):
            peak = jnp.maximum(peak, energy[:, b * LANES : (b + 1) * LANES])
        span = LANES // 2
        while span >= half:
            peak = jnp.maximum(peak, pltpu.roll(peak, span, 1))
            span //= 2
        peak = peak / cnorm[...]
        lane = lax.broadcasted_iota(jnp.int32, (cq, LANES), 1) // segs
        for i in range(4):
            src = source(4 * g + i)
            moved = pltpu.roll(peak, lax.rem(src * segs + LANES - i * segs, LANES), 1)
            cres[...] = jnp.where(lane == src, moved, cres[...])

    def fine_peak(g):
        total = fstage[g, fx]
        for k in range(1, nf):
            fx_move(g, k).wait_recv()
            total = total + frecv[g, k - 1]
        energy = total[:fq] * total[:fq] + total[fq:] * total[fq:]
        peak = energy
        span = LANES // 2
        while span >= 8:
            peak = jnp.maximum(peak, pltpu.roll(peak, span, 1))
            span //= 2
        peak = peak / fnorm[...]
        square = jnp.concatenate([peak, jnp.zeros((LANES - fq, LANES), jnp.float32)], axis=0)
        rstage[g] = square.T[:8]

    def norms():
        total = nstage[fx]
        for k in range(1, nf):
            n_move(k).wait_recv()
            total = total + nrecv[k - 1]
        cnorm[...] = total[:cq]
        fnorm[...] = total[cq:]
        cres[...] = jnp.zeros_like(cres)

    def give_back(g):
        for p in range(4 * g, 4 * g + 4):
            if p > 0:
                r_move(p).start()

    for g in range(groups):
        here = (4 * g + 1, 4 * g + 2)
        for p in here:
            c_move(p).wait_recv()
            if p + 2 <= nb - 1:
                c_move(p + 2).start()
        for c in range(parts):
            for p in here:
                f_move(p, c).wait_recv()
                if p + 2 <= nb - 1 and not (p + 2 == nb - 1 and c >= parts // 2):
                    f_move(p + 2, c).start()
                if p + 1 == nb - 1 and c >= parts // 2:
                    f_move(p + 1, c).start()
        if g == 0:
            powers()
        else:
            if g == 1:
                norms()
            coarse_peak(g - 1)
            fine_peak(g - 1)
            give_back(g - 1)
        last = g == groups - 1
        here = [p for p in (4 * g + 3, 4 * g + 4) if p <= nb - 1]
        for p in here:
            c_move(p).wait_recv()
            if p + 2 <= nb - 1:
                c_move(p + 2).start()
        coarse_group(g)
        fpq[...] = jnp.zeros_like(fpq)

        def piece(i, carry, g=g, here=here, last=last):
            c = (i % 2) * (parts // 2) + i // 2 if last else i
            for p in here:
                f_move(p, c).wait_recv()
                if not last:
                    f_move(p + 2, c).start()
            fine_piece(g, c)

            @pl.when(i == 0)
            def _():
                for k in range(1, nf):
                    cx_move(g, k).start()
                if g == 0:
                    for k in range(1, nf):
                        n_move(k).start()

            return carry

        lax.fori_loop(0, parts, piece, 0)
        fine_done(g)
        for k in range(1, nf):
            fx_move(g, k).start()
    if groups == 1:
        norms()
    coarse_peak(groups - 1)
    fine_peak(groups - 1)
    give_back(groups - 1)
    coarse_out[...] = cres[...]
    rrecv[0] = rstage[0]
    for p in range(1, nb):
        r_move(p).wait_recv()

    result = jnp.zeros((8, LANES), jnp.float32)
    named = []
    for s in range(segs):
        for k in range(2):
            bank = trig[k, me * segs + s]
            rank = jnp.int32(0)
            for before in named:
                rank = rank + jnp.where(before == bank, 1, 0)
            named.append(bank)
            away = lax.rem(me - bank + nb, nb)
            place = jnp.where(away < nb // 2, 2 * away, 2 * (nb - away) - 1)
            row = lax.rem(place, 4) * 2 + rank
            tile = rrecv[place]
            line = jnp.sum(jnp.where(orow == row, tile, 0.0), axis=0, keepdims=True)
            result = jnp.where(orow == 2 * s + k, line, result)
    fine_out[...] = result

    for p in range(1, nb):
        c_move(p).wait_send()
        for c in range(parts):
            f_move(p, c).wait_send()
        r_move(p).wait_send()
    for k in range(1, nf):
        n_move(k).wait_send()
        for g in range(groups):
            cx_move(g, k).wait_send()
            fx_move(g, k).wait_send()


def body(
    nb,
    nf,
    coarse_spectra,
    fine_spectra,
    coarse_templates,
    fine_templates,
    coarse_weight,
    fine_weight,
    triggers,
    offsets,
):
    segs, _, cbins = coarse_spectra.shape
    fbins = fine_spectra.shape[2]
    ctn = coarse_templates.shape[1]
    ftn = fine_templates.shape[2]
    groups = nb // 4
    parts = 4
    cq, fq = ctn // nf, ftn // nf
    ccol, fcol = LC * 4 * segs, LF * 8
    f32, bf16 = jnp.float32, jnp.bfloat16
    dma = pltpu.SemaphoreType.DMA
    anywhere = pl.BlockSpec(memory_space=pl.ANY)
    smem = pl.BlockSpec(memory_space=pltpu.SMEM)
    vmem = pl.BlockSpec(memory_space=pltpu.VMEM)
    coarse, fine = pl.pallas_call(
        functools.partial(kernel, nb, nf),
        out_shape=(
            jax.ShapeDtypeStruct((cq, LANES), f32),
            jax.ShapeDtypeStruct((8, LANES), f32),
        ),
        in_specs=[smem, smem] + [anywhere] * 6,
        out_specs=(vmem, vmem),
        scratch_shapes=[
            pltpu.VMEM((segs, 2, cbins), bf16),
            pltpu.VMEM((segs, 2, fbins), bf16),
            pltpu.VMEM((nb, 2 * segs, cbins), bf16),
            pltpu.VMEM((nb, 2 * segs, fbins), bf16),
            pltpu.VMEM((2 * ctn, cbins), bf16),
            pltpu.VMEM((2 * ftn, fbins), bf16),
            pltpu.VMEM((1, cbins), f32),
            pltpu.VMEM((1, fbins), f32),
            pltpu.VMEM((8 * segs, cbins), f32),
            pltpu.VMEM((16, fbins // parts), f32),
            pltpu.VMEM((2, LC, cbins), f32),
            pltpu.VMEM((2, LF, fbins), f32),
            pltpu.VMEM((2 * ccol, min(DEEP, cbins)), bf16),
            pltpu.VMEM((2 * fcol, min(DEEP, fbins // parts)), bf16),
            pltpu.VMEM((2 * ccol, 2 * ctn), f32),
            pltpu.VMEM((2 * fcol, 2 * ftn), f32),
            pltpu.VMEM((groups, 16, 8 * segs), bf16),
            pltpu.VMEM((groups, 8, LANES), jnp.int32),
            pltpu.VMEM((groups, nf, 2 * cq, ccol), f32),
            pltpu.VMEM((groups, nf - 1, 2 * cq, ccol), f32),
            pltpu.VMEM((groups, nf, 2 * fq, fcol), f32),
            pltpu.VMEM((groups, nf - 1, 2 * fq, fcol), f32),
            pltpu.VMEM((nf, cq + fq, LANES), f32),
            pltpu.VMEM((nf - 1, cq + fq, LANES), f32),
            pltpu.VMEM((cq, LANES), f32),
            pltpu.VMEM((fq, LANES), f32),
            pltpu.VMEM((cq, LANES), f32),
            pltpu.VMEM((groups, 8, LANES), f32),
            pltpu.VMEM((nb, 8, LANES), f32),
            dma((2,)),
            dma((2,)),
            dma,
            dma,
            dma((nb,)),
            dma((nb,)),
            dma((nb, parts)),
            dma((nb, parts)),
            dma((nf - 1,)),
            dma((nf - 1,)),
            dma((groups, nf - 1)),
            dma((groups, nf - 1)),
            dma((groups, nf - 1)),
            dma((groups, nf - 1)),
            dma((nb,)),
            dma((nb,)),
        ],
        compiler_params=pltpu.CompilerParams(
            collective_id=0, has_side_effects=True, vmem_limit_bytes=67043328
        ),
        name="search",
    )(
        triggers.T,
        offsets.T,
        coarse_spectra,
        fine_spectra,
        coarse_templates.reshape(2 * ctn, cbins),
        fine_templates.reshape(2 * ftn, fbins),
        coarse_weight.reshape(1, cbins),
        fine_weight.reshape(1, fbins),
    )
    coarse_snr = coarse[:, : nb * segs]
    fine_snr = fine[:, :fq].reshape(segs, 2, fq)
    return coarse_snr, fine_snr


def solution(mesh):
    return jax.shard_map(
        functools.partial(body, mesh.shape["bank"], mesh.shape["freq"]),
        mesh=mesh,
        in_specs=(
            P(("groups", "seg", "bank"), None, "freq"),
            P(("groups", "seg", "bank"), None, "freq"),
            P(None, "bank", "freq"),
            P(None, "bank", None, "freq"),
            P(("groups", "freq")),
            P(("groups", "freq")),
            P(("groups", "seg"), None),
            P(("groups", "seg"), None),
        ),
        out_specs=(
            P(("bank", "freq"), ("groups", "seg")),
            P(("groups", "seg", "bank"), None, "freq"),
        ),
        check_vma=False,
    )
```

```python
import functools
import math

import jax
import jax.numpy as jnp
from jax import lax
from jax.experimental import pallas as pl
from jax.experimental.pallas import tpu as pltpu
from jax.sharding import PartitionSpec as P

FC = 16384
FB = 65536
CAP = 2
LC = 16
LF = 16
CSTRIDE = 2047
PERIOD = 131072
STEP = 512
DEEP = 2048
LANES = 128
MESH = pl.DeviceIdType.MESH
NT = (((1,), (1,)), ((), ()))
NN = (((1,), (0,)), ((), ()))


def unit_phase(count):
    quadrant = (count + PERIOD // 8) >> 15
    x = (count - (quadrant << 15)).astype(jnp.float32) * (2.0 * math.pi / PERIOD)
    z = x * x
    s = x * (1.0 + z * (-1.0 / 6 + z * (1.0 / 120 + z * (-1.0 / 5040 + z * (1.0 / 362880)))))
    c = 1.0 + z * (-0.5 + z * (1.0 / 24 + z * (-1.0 / 720 + z * (1.0 / 40320 - z * (1.0 / 3628800)))))
    odd = (quadrant & 1) == 1
    cos = jnp.where(odd, s, c)
    sin = jnp.where(odd, c, s)
    cos = jnp.where(((quadrant + 1) & 2) == 2, -cos, cos)
    sin = jnp.where((quadrant & 2) == 2, -sin, sin)
    return cos, sin


def kernel(
    nb,
    nf,
    trig,
    offs,
    cs_hbm,
    fs_hbm,
    ct_hbm,
    ft_hbm,
    cw_hbm,
    fw_hbm,
    coarse_out,
    fine_out,
    craw,
    fraw,
    cbuf,
    fbuf,
    ct,
    ft,
    cw,
    fw,
    stab,
    cpure,
    fpure,
    ctab,
    ftab,
    clag,
    flag,
    cpq,
    fpq,
    sel,
    soff,
    cstage,
    crecv,
    fstage,
    frecv,
    nstage,
    nrecv,
    cnorm,
    fnorm,
    cres,
    rstage,
    rrecv,
    load_sem,
    w_sem,
    ct_sem,
    ft_sem,
    c_send,
    c_recv,
    f_send,
    f_recv,
    n_send,
    n_recv,
    cx_send,
    cx_recv,
    fx_send,
    fx_recv,
    r_send,
    r_recv,
):
    me = lax.axis_index("bank")
    fx = lax.axis_index("freq")
    groups = nb // 4
    segs = cbuf.shape[1] // 2
    cbins = cbuf.shape[2]
    fbins = fbuf.shape[2]
    parts = f_send.shape[1]
    fpart = fbins // parts
    ctn = ct.shape[0] // 2
    ftn = ft.shape[0] // 2
    cq = ctn // nf
    fq = ftn // nf
    scale = PERIOD // (2 * FC)

    def source(p):
        step = (nb - (p + 1) // 2) if p % 2 else p // 2
        return lax.rem(me + step, nb)

    def other(k):
        return lax.rem(fx + k, nf)

    right = lax.rem(me + 1, nb)
    left = lax.rem(me + nb - 1, nb)

    def c_move(p):
        return pltpu.make_async_remote_copy(
            src_ref=cbuf.at[max(p - 2, 0)],
            dst_ref=cbuf.at[p],
            send_sem=c_send.at[p],
            recv_sem=c_recv.at[p],
            device_id={"bank": right if p % 2 else left},
            device_id_type=MESH,
        )

    def f_move(p, c, leftward=None):
        if leftward is None:
            leftward = p % 2 == 0
        origin = p - 1 if (p == nb - 1 and leftward) else max(p - 2, 0)
        part = pl.ds(pl.multiple_of(c * fpart, fpart), fpart)
        return pltpu.make_async_remote_copy(
            src_ref=fbuf.at[origin, :, part],
            dst_ref=fbuf.at[p, :, part],
            send_sem=f_send.at[p, c],
            recv_sem=f_recv.at[p, c],
            device_id={"bank": left if leftward else right},
            device_id_type=MESH,
        )

    def n_move(k):
        return pltpu.make_async_remote_copy(
            src_ref=nstage.at[other(k)],
            dst_ref=nrecv.at[k - 1],
            send_sem=n_send.at[k - 1],
            recv_sem=n_recv.at[k - 1],
            device_id={"freq": other(k)},
            device_id_type=MESH,
        )

    def cx_move(g, k):
        return pltpu.make_async_remote_copy(
            src_ref=cstage.at[g, other(k)],
            dst_ref=crecv.at[g, k - 1],
            send_sem=cx_send.at[g, k - 1],
            recv_sem=cx_recv.at[g, k - 1],
            device_id={"freq": other(k)},
            device_id_type=MESH,
        )

    def fx_move(g, k):
        return pltpu.make_async_remote_copy(
            src_ref=fstage.at[g, other(k)],
            dst_ref=frecv.at[g, k - 1],
            send_sem=fx_send.at[g, k - 1],
            recv_sem=fx_recv.at[g, k - 1],
            device_id={"freq": other(k)},
            device_id_type=MESH,
        )

    def r_move(p):
        return pltpu.make_async_remote_copy(
            src_ref=rstage.at[p // 4 if p < nb - 1 else groups],
            dst_ref=rrecv.at[p],
            send_sem=r_send.at[p],
            recv_sem=r_recv.at[p],
            device_id={"bank": source(p)},
            device_id_type=MESH,
        )

    own_c = pltpu.make_async_copy(cs_hbm, craw, load_sem.at[0])
    own_f = pltpu.make_async_copy(fs_hbm, fraw, load_sem.at[1])
    own_c.start()
    own_f.start()
    load_cw = pltpu.make_async_copy(cw_hbm, cw, w_sem.at[0])
    load_fw = pltpu.make_async_copy(fw_hbm, fw, w_sem.at[1])
    load_cw.start()
    load_fw.start()
    load_ct = pltpu.make_async_copy(ct_hbm, ct, ct_sem)
    load_ft = pltpu.make_async_copy(ft_hbm, ft, ft_sem)
    load_ct.start()
    load_ft.start()

    barrier = pltpu.get_barrier_semaphore()
    for neighbour in (left, right):
        pl.semaphore_signal(barrier, inc=1, device_id={"bank": neighbour}, device_id_type=MESH)
    for k in range(1, nf):
        pl.semaphore_signal(barrier, inc=1, device_id={"freq": other(k)}, device_id_type=MESH)
    own_c.wait()
    own_f.wait()

    def settle(raw, buf, begin, size):
        for at in range(begin, begin + size, STEP):
            piece = [raw[r, :, at : at + STEP].astype(jnp.float32) for r in range(segs)]
            buf[0, :, at : at + STEP] = jnp.concatenate(piece, axis=0).astype(jnp.bfloat16)

    settle(fraw, fbuf, 0, fpart)
    pl.semaphore_wait(barrier, 2 + nf - 1)
    for c in range(parts):
        if c + 1 < parts:
            settle(fraw, fbuf, (c + 1) * fpart, fpart)
        else:
            settle(craw, cbuf, 0, cbins)
        for p in (1, 2):
            f_move(p, c).start()
    for p in (1, 2):
        c_move(p).start()
    load_cw.wait()
    load_fw.wait()

    def c_phases(i, carry):
        at = pl.ds(pl.multiple_of(i * STEP, STEP), STEP)
        lag = lax.broadcasted_iota(jnp.int32, (LC, STEP), 0) * CSTRIDE
        f = fx * cbins + i * STEP + lax.broadcasted_iota(jnp.int32, (LC, STEP), 1)
        cos, sin = unit_phase((f * lag * scale) & (PERIOD - 1))
        w = cw[:, at]
        ctab[0, :, at] = cos * w
        ctab[1, :, at] = sin * w
        return carry

    lax.fori_loop(0, cbins // STEP, c_phases, 0)

    def f_phases(i, carry):
        at = pl.ds(pl.multiple_of(i * STEP, STEP), STEP)
        lag = lax.broadcasted_iota(jnp.int32, (LF, STEP), 0)
        f = fx * fbins + i * STEP + lax.broadcasted_iota(jnp.int32, (LF, STEP), 1)
        cos, sin = unit_phase((f * lag) & (PERIOD - 1))
        w = fw[:, at]
        ftab[0, :, at] = cos * w
        ftab[1, :, at] = sin * w
        return carry

    lax.fori_loop(0, fbins // STEP, f_phases, 0)

    def single_phases():
        def step(i, carry):
            at = pl.ds(pl.multiple_of(i * STEP, STEP), STEP)
            lag = lax.broadcasted_iota(jnp.int32, (2 * LF, STEP), 0) // 2
            f = fx * fbins + i * STEP + lax.broadcasted_iota(jnp.int32, (2 * LF, STEP), 1)
            cos, sin = unit_phase((f * lag) & (PERIOD - 1))
            w = fw[:, at]
            stab[0, :, at] = cos * w
            stab[1, :, at] = sin * w
            return carry

        lax.fori_loop(0, fbins // STEP, step, 0)

    rows = lax.broadcasted_iota(jnp.int32, (16, 8 * segs), 0)
    cols = lax.broadcasted_iota(jnp.int32, (16, 8 * segs), 1)
    orow = lax.broadcasted_iota(jnp.int32, (8, LANES), 0)
    units = [list(range(4 * g, min(4 * g + 4, nb - 1))) for g in range(groups)] + [[nb - 1]]
    for u, places in enumerate(units):
        pick = jnp.zeros((16, 8 * segs), jnp.float32)
        shift = jnp.zeros((8, LANES), jnp.int32)
        for i, p in enumerate(places):
            base = source(p) * segs
            found = jnp.int32(0)
            for s in range(segs):
                for k in range(2):
                    hit = jnp.where(trig[k, base + s] == me, 1, 0)
                    slot = 2 * i + found
                    row = (rows & 7) & 1 if u == groups else rows & 7
                    col = (i * segs + s) * 2
                    here = (row == slot) & (cols == col + (rows >> 3))
                    pick += jnp.where(here, hit.astype(jnp.float32), 0.0)
                    shift += jnp.where((orow & 1 if u == groups else orow) == slot, hit * offs[k, base + s], 0)
                    found = found + hit
        sel[u] = pick.astype(jnp.bfloat16)
        soff[u] = shift

    def powers():
        load_ct.wait()

        def c_power(i, total):
            at = pl.ds(pl.multiple_of(i * LANES, LANES), LANES)
            re = ct[:ctn, at].astype(jnp.float32)
            im = ct[ctn:, at].astype(jnp.float32)
            return total + (re * re + im * im) * cw[:, at]

        ct_sum = lax.fori_loop(0, cbins // LANES, c_power, jnp.zeros((ctn, LANES), jnp.float32))
        ct_sum = jnp.broadcast_to(jnp.sum(ct_sum, axis=1, keepdims=True), (ctn, LANES))
        load_ft.wait()

        def f_power(i, total):
            at = pl.ds(pl.multiple_of(i * LANES, LANES), LANES)
            re = ft[:ftn, at].astype(jnp.float32)
            im = ft[ftn:, at].astype(jnp.float32)
            return total + (re * re + im * im) * fw[:, at]

        ft_sum = lax.fori_loop(0, fbins // LANES, f_power, jnp.zeros((ftn, LANES), jnp.float32))
        ft_sum = jnp.broadcast_to(jnp.sum(ft_sum, axis=1, keepdims=True), (ftn, LANES))
        for q in range(nf):
            nstage[q, :cq] = ct_sum[q * cq : (q + 1) * cq]
            nstage[q, cq:] = ft_sum[q * fq : (q + 1) * fq]

    def coarse_group(g):
        half = 4 * segs
        prow = lax.broadcasted_iota(jnp.int32, (2 * half, 2 * half), 0)
        pcol = lax.broadcasted_iota(jnp.int32, (2 * half, 2 * half), 1)
        want = jnp.where(prow < half, 2 * prow, 2 * (prow - half) + 1)
        split = jnp.where(pcol == want, 1.0, 0.0).astype(jnp.bfloat16)
        ncol = LC * half
        wide = min(2 * STEP, cbins)
        for begin in range(0, cbins, wide):
            at = slice(begin, begin + wide)
            block = jnp.concatenate([cbuf[4 * g + b, :, at].astype(jnp.float32) for b in range(4)], axis=0)
            cpure[:, at] = lax.dot_general(split, block.astype(jnp.bfloat16), NN, preferred_element_type=jnp.float32)
        cpq[...] = jnp.zeros_like(cpq)
        deep = min(DEEP, cbins)

        def step(i, carry):
            base = pl.multiple_of(i * deep, deep)
            for kt in range(0, deep, 2 * LANES):
                at = pl.ds(base + kt, 2 * LANES)
                yr, yi = cpure[:half, at], cpure[half:, at]
                for j in range(LC):
                    c = ctab[0, j : j + 1, at]
                    s = ctab[1, j : j + 1, at]
                    clag[j * half : (j + 1) * half, kt : kt + 2 * LANES] = (yr * c - yi * s).astype(jnp.bfloat16)
                    clag[ncol + j * half : ncol + (j + 1) * half, kt : kt + 2 * LANES] = (yr * s + yi * c).astype(jnp.bfloat16)
            cpq[...] += lax.dot_general(clag[...], ct[:, pl.ds(base, deep)], NT, preferred_element_type=jnp.float32)
            return carry

        lax.fori_loop(0, cbins // deep, step, 0)
        re = (cpq[:ncol, :ctn] + cpq[ncol:, ctn:]).T
        im = (cpq[ncol:, :ctn] - cpq[:ncol, ctn:]).T
        for q in range(nf):
            cstage[g, q, :cq] = re[q * cq : (q + 1) * cq]
            cstage[g, q, cq:] = im[q * cq : (q + 1) * cq]

    def fine_piece(u, c):
        single = u == groups
        ncol = LF * (2 if single else 8)
        table = stab if single else ftab
        places = units[u] + (units[groups - 1] if single else [])
        places = (places + places)[:4]
        wide = min(2 * STEP, fpart)
        for begin in range(0, fpart, wide):
            first = c * fpart + begin
            at = pl.ds(pl.multiple_of(first, wide), wide)
            block = jnp.concatenate([fbuf[p, :, at].astype(jnp.float32) for p in places], axis=0)
            y = lax.dot_general(sel[u], block.astype(jnp.bfloat16), NN, preferred_element_type=jnp.float32)
            f = fx * fbins + first + lax.broadcasted_iota(jnp.int32, (8, wide), 1)
            shift = jnp.concatenate([soff[u]] * (wide // LANES), axis=1)
            cos, sin = unit_phase((f * shift) & (PERIOD - 1))
            yr, yi = y[:8], y[8:]
            fpure[:8, begin : begin + wide] = yr * cos - yi * sin
            fpure[8:, begin : begin + wide] = yr * sin + yi * cos
        deep = min(DEEP, fpart)

        def step(i, carry):
            base = pl.multiple_of(i * deep, deep)
            whole = pl.multiple_of(c * fpart + i * deep, deep)
            for kt in range(0, deep, 2 * LANES):
                sr = fpure[:8, pl.ds(base + kt, 2 * LANES)]
                si = fpure[8:, pl.ds(base + kt, 2 * LANES)]
                at = pl.ds(whole + kt, 2 * LANES)
                here = slice(kt, kt + 2 * LANES)
                for j in range(0, ncol // 8, 2):
                    res, ims = [], []
                    for jj in (j, j + 1):
                        lag = slice(jj * 8, jj * 8 + 8) if single else slice(jj, jj + 1)
                        wc = table[0, lag, at]
                        ws = table[1, lag, at]
                        res.append(sr * wc - si * ws)
                        ims.append(sr * ws + si * wc)
                    flag[j * 8 : j * 8 + 16, here] = jnp.concatenate(res, axis=0).astype(jnp.bfloat16)
                    flag[ncol + j * 8 : ncol + j * 8 + 16, here] = jnp.concatenate(ims, axis=0).astype(jnp.bfloat16)
            fpq[: 2 * ncol] += lax.dot_general(
                flag[: 2 * ncol], ft[:, pl.ds(whole, deep)], NT, preferred_element_type=jnp.float32
            )
            return carry

        lax.fori_loop(0, fpart // deep, step, 0)

    def fine_done(u):
        ncol = LF * (2 if u == groups else 8)
        top, bottom = fpq[:ncol], fpq[ncol : 2 * ncol]
        re = top + pltpu.roll(bottom, ftn, 1)
        im = bottom - pltpu.roll(top, ftn, 1)
        if ncol < LANES:
            rest = jnp.zeros((LANES - ncol, LANES), jnp.float32)
            re = jnp.concatenate([re, rest], axis=0)
            im = jnp.concatenate([im, rest], axis=0)
        re, im = re.T, im.T
        for q in range(nf):
            fstage[u, q, :fq] = re[q * fq : (q + 1) * fq]
            fstage[u, q, fq:] = im[q * fq : (q + 1) * fq]

    def coarse_peak(g):
        total = cstage[g, fx]
        for k in range(1, nf):
            cx_move(g, k).wait_recv()
            total = total + crecv[g, k - 1]
        energy = total[:cq] * total[:cq] + total[cq:] * total[cq:]
        half = 4 * segs
        peak = energy[:, :LANES]
        for b in range(1, LC * half // LANES):
            peak = jnp.maximum(peak, energy[:, b * LANES : (b + 1) * LANES])
        span = LANES // 2
        while span >= half:
            peak = jnp.maximum(peak, pltpu.roll(peak, span, 1))
            span //= 2
        peak = peak / cnorm[...]
        lane = lax.broadcasted_iota(jnp.int32, (cq, LANES), 1) // segs
        for i in range(4):
            src = source(4 * g + i)
            moved = pltpu.roll(peak, lax.rem(src * segs + LANES - i * segs, LANES), 1)
            cres[...] = jnp.where(lane == src, moved, cres[...])

    def fine_peak(g):
        total = fstage[g, fx]
        for k in range(1, nf):
            fx_move(g, k).wait_recv()
            total = total + frecv[g, k - 1]
        energy = total[:fq] * total[:fq] + total[fq:] * total[fq:]
        peak = energy
        least, span = (2, LF) if g == groups else (8, LANES // 2)
        while span >= least:
            peak = jnp.maximum(peak, pltpu.roll(peak, LANES - span, 1))
            span //= 2
        peak = peak / fnorm[...]
        square = jnp.concatenate([peak, jnp.zeros((LANES - fq, LANES), jnp.float32)], axis=0)
        rstage[g] = square.T[:8]

    def norms():
        total = nstage[fx]
        for k in range(1, nf):
            n_move(k).wait_recv()
            total = total + nrecv[k - 1]
        cnorm[...] = total[:cq]
        fnorm[...] = total[cq:]
        cres[...] = jnp.zeros_like(cres)

    def give_back(u):
        for p in units[u]:
            if p > 0:
                r_move(p).start()

    def start_all(move, g):
        for k in range(1, nf):
            move(g, k).start()

    def hop(h, unit=None, first=None):
        here = [p for p in (2 * h - 1, 2 * h) if p <= nb - 1]
        half = parts // 2
        if unit is not None:
            fpq[...] = jnp.zeros_like(fpq)

        def part(i, carry):
            c = (i % 2) * half + i // 2 if here == [nb - 1] else i
            for p in here:
                f_move(p, c).wait_recv()
                if p + 2 < nb - 1:
                    f_move(p + 2, c).start()
                elif p + 2 == nb - 1:

                    @pl.when(c < half)
                    def _():
                        f_move(nb - 1, c, leftward=False).start()

                elif p + 1 == nb - 1:

                    @pl.when(c >= half)
                    def _():
                        f_move(nb - 1, c, leftward=True).start()

            if first is not None:

                @pl.when(i == 0)
                def _():
                    first()

            if unit is not None:
                fine_piece(unit, c)
            return carry

        lax.fori_loop(0, parts, part, 0)
        if unit is not None:
            fine_done(unit)
            start_all(fx_move, unit)

    def pass_coarse(h):
        for p in (2 * h - 1, 2 * h):
            if p <= nb - 1:
                c_move(p).wait_recv()
                if p + 2 <= nb - 1:
                    c_move(p + 2).start()

    if groups == 1:
        powers()
        single_phases()
        for k in range(1, nf):
            n_move(k).start()
    for g in range(groups - 1):
        hop(2 * g + 1, first=functools.partial(start_all, cx_move, g - 1) if g else None)
        pass_coarse(2 * g + 1)
        if g == 0:
            powers()
        else:
            if g == 1:
                norms()
                single_phases()
            fine_peak(g - 1)
            give_back(g - 1)
            coarse_peak(g - 1)
        hop(2 * g + 2, g)
        pass_coarse(2 * g + 2)
        if g == 0:
            for k in range(1, nf):
                n_move(k).start()
        coarse_group(g)
    if groups == 2:
        single_phases()
    last = groups - 1
    hop(2 * last + 1, last, functools.partial(start_all, cx_move, last - 1) if last else None)
    pass_coarse(2 * last + 1)
    hop(2 * last + 2, groups)
    if groups <= 2:
        norms()
    if last:
        fine_peak(last - 1)
        give_back(last - 1)
    fine_peak(last)
    give_back(last)
    pass_coarse(2 * last + 2)
    coarse_group(last)
    fine_peak(groups)
    give_back(groups)
    start_all(cx_move, last)
    rrecv[0] = rstage[0]
    if last:
        coarse_peak(last - 1)
    for p in range(1, nb):
        c_move(p).wait_send()
        for c in range(parts):
            f_move(p, c).wait_send()
    for k in range(1, nf):
        n_move(k).wait_send()
        for g in range(groups + 1):
            fx_move(g, k).wait_send()
            if g < last:
                cx_move(g, k).wait_send()
    coarse_peak(last)
    coarse_out[...] = cres[...]
    for p in range(1, nb):
        r_move(p).wait_recv()

    result = jnp.zeros((8, LANES), jnp.float32)
    named = []
    for s in range(segs):
        for k in range(2):
            bank = trig[k, me * segs + s]
            rank = jnp.int32(0)
            for before in named:
                rank = rank + jnp.where(before == bank, 1, 0)
            named.append(bank)
            away = lax.rem(me - bank + nb, nb)
            place = jnp.where(away < nb // 2, 2 * away, 2 * (nb - away) - 1)
            row = jnp.where(place == nb - 1, 0, lax.rem(place, 4) * 2) + rank
            tile = rrecv[place]
            line = jnp.sum(jnp.where(orow == row, tile, 0.0), axis=0, keepdims=True)
            result = jnp.where(orow == 2 * s + k, line, result)
    fine_out[...] = result

    for p in range(1, nb):
        r_move(p).wait_send()
    for k in range(1, nf):
        cx_move(last, k).wait_send()


def body(
    nb,
    nf,
    coarse_spectra,
    fine_spectra,
    coarse_templates,
    fine_templates,
    coarse_weight,
    fine_weight,
    triggers,
    offsets,
):
    segs, _, cbins = coarse_spectra.shape
    fbins = fine_spectra.shape[2]
    ctn = coarse_templates.shape[1]
    ftn = fine_templates.shape[2]
    groups = nb // 4
    parts = 4
    cq, fq = ctn // nf, ftn // nf
    ccol, fcol = LC * 4 * segs, LF * 8
    f32, bf16 = jnp.float32, jnp.bfloat16
    dma = pltpu.SemaphoreType.DMA
    anywhere = pl.BlockSpec(memory_space=pltpu.HBM)
    smem = pl.BlockSpec(memory_space=pltpu.SMEM)
    vmem = pl.BlockSpec(memory_space=pltpu.VMEM)
    coarse, fine = pl.pallas_call(
        functools.partial(kernel, nb, nf),
        out_shape=(
            jax.ShapeDtypeStruct((cq, LANES), f32),
            jax.ShapeDtypeStruct((8, LANES), f32),
        ),
        in_specs=[smem, smem] + [anywhere] * 6,
        out_specs=(vmem, vmem),
        scratch_shapes=[
            pltpu.VMEM((segs, 2, cbins), bf16),
            pltpu.VMEM((segs, 2, fbins), bf16),
            pltpu.VMEM((nb, 2 * segs, cbins), bf16),
            pltpu.VMEM((nb, 2 * segs, fbins), bf16),
            pltpu.VMEM((2 * ctn, cbins), bf16),
            pltpu.VMEM((2 * ftn, fbins), bf16),
            pltpu.VMEM((1, cbins), f32),
            pltpu.VMEM((1, fbins), f32),
            pltpu.VMEM((2, 2 * LF, fbins), f32),
            pltpu.VMEM((8 * segs, cbins), f32),
            pltpu.VMEM((16, fbins // parts), f32),
            pltpu.VMEM((2, LC, cbins), f32),
            pltpu.VMEM((2, LF, fbins), f32),
            pltpu.VMEM((2 * ccol, min(DEEP, cbins)), bf16),
            pltpu.VMEM((2 * fcol, min(DEEP, fbins // parts)), bf16),
            pltpu.VMEM((2 * ccol, 2 * ctn), f32),
            pltpu.VMEM((2 * fcol, 2 * ftn), f32),
            pltpu.VMEM((groups + 1, 16, 8 * segs), bf16),
            pltpu.VMEM((groups + 1, 8, LANES), jnp.int32),
            pltpu.VMEM((groups, nf, 2 * cq, ccol), f32),
            pltpu.VMEM((groups, nf - 1, 2 * cq, ccol), f32),
            pltpu.VMEM((groups + 1, nf, 2 * fq, fcol), f32),
            pltpu.VMEM((groups + 1, nf - 1, 2 * fq, fcol), f32),
            pltpu.VMEM((nf, cq + fq, LANES), f32),
            pltpu.VMEM((nf - 1, cq + fq, LANES), f32),
            pltpu.VMEM((cq, LANES), f32),
            pltpu.VMEM((fq, LANES), f32),
            pltpu.VMEM((cq, LANES), f32),
            pltpu.VMEM((groups + 1, 8, LANES), f32),
            pltpu.VMEM((nb, 8, LANES), f32),
            dma((2,)),
            dma((2,)),
            dma,
            dma,
            dma((nb,)),
            dma((nb,)),
            dma((nb, parts)),
            dma((nb, parts)),
            dma((nf - 1,)),
            dma((nf - 1,)),
            dma((groups, nf - 1)),
            dma((groups, nf - 1)),
            dma((groups + 1, nf - 1)),
            dma((groups + 1, nf - 1)),
            dma((nb,)),
            dma((nb,)),
        ],
        compiler_params=pltpu.CompilerParams(
            collective_id=0, has_side_effects=True, vmem_limit_bytes=40 * 1024 * 1024
        ),
        name="search",
    )(
        triggers.T,
        offsets.T,
        coarse_spectra,
        fine_spectra,
        coarse_templates.reshape(2 * ctn, cbins),
        fine_templates.reshape(2 * ftn, fbins),
        coarse_weight.reshape(1, cbins),
        fine_weight.reshape(1, fbins),
    )
    coarse_snr = coarse[:, : nb * segs]
    fine_snr = fine[:, :fq].reshape(segs, 2, fq)
    return coarse_snr, fine_snr


def solution(mesh):
    return jax.shard_map(
        functools.partial(body, mesh.shape["bank"], mesh.shape["freq"]),
        mesh=mesh,
        in_specs=(
            P(("groups", "seg", "bank"), None, "freq"),
            P(("groups", "seg", "bank"), None, "freq"),
            P(None, "bank", "freq"),
            P(None, "bank", None, "freq"),
            P(("groups", "freq")),
            P(("groups", "freq")),
            P(("groups", "seg"), None),
            P(("groups", "seg"), None),
        ),
        out_specs=(
            P(("bank", "freq"), ("groups", "seg")),
            P(("groups", "seg", "bank"), None, "freq"),
        ),
        check_vma=False,
    )
```

```python
import functools
import math

import jax
import jax.numpy as jnp
from jax import lax
from jax.experimental import pallas as pl
from jax.experimental.pallas import tpu as pltpu
from jax.sharding import PartitionSpec as P

FC = 16384
FB = 65536
CAP = 2
LC = 16
LF = 16
CSTRIDE = 2047
PERIOD = 131072
STEP = 512
DEEP = 2048
LANES = 128
MESH = pl.DeviceIdType.MESH
NT = (((1,), (1,)), ((), ()))
NN = (((1,), (0,)), ((), ()))


def unit_phase(count):
    quadrant = (count + PERIOD // 8) >> 15
    x = (count - (quadrant << 15)).astype(jnp.float32) * (2.0 * math.pi / PERIOD)
    z = x * x
    s = x * (1.0 + z * (-1.0 / 6 + z * (1.0 / 120 + z * (-1.0 / 5040 + z * (1.0 / 362880)))))
    c = 1.0 + z * (-0.5 + z * (1.0 / 24 + z * (-1.0 / 720 + z * (1.0 / 40320 - z * (1.0 / 3628800)))))
    odd = (quadrant & 1) == 1
    cos = jnp.where(odd, s, c)
    sin = jnp.where(odd, c, s)
    cos = jnp.where(((quadrant + 1) & 2) == 2, -cos, cos)
    sin = jnp.where((quadrant & 2) == 2, -sin, sin)
    return cos, sin


def kernel(
    nb,
    nf,
    trig,
    offs,
    cs_hbm,
    fs_hbm,
    ct_hbm,
    ft_hbm,
    cw_hbm,
    fw_hbm,
    coarse_out,
    fine_out,
    craw,
    fraw,
    cbuf,
    fbuf,
    ct,
    ft,
    cw,
    fw,
    cpure,
    fpure,
    ctab,
    ftab,
    clag,
    flag,
    cpq,
    fpq,
    sel,
    soff,
    cstage,
    crecv,
    fstage,
    frecv,
    nstage,
    nrecv,
    cnorm,
    fnorm,
    cres,
    rstage,
    rrecv,
    load_sem,
    w_sem,
    ct_sem,
    ft_sem,
    c_send,
    c_recv,
    f_send,
    f_recv,
    n_send,
    n_recv,
    cx_send,
    cx_recv,
    fx_send,
    fx_recv,
    r_send,
    r_recv,
):
    me = lax.axis_index("bank")
    fx = lax.axis_index("freq")
    groups = nb // 4
    segs = cbuf.shape[1] // 2
    cbins = cbuf.shape[2]
    fbins = fbuf.shape[2]
    parts = f_send.shape[1]
    fpart = fbins // parts
    ctn = ct.shape[0] // 2
    ftn = ft.shape[0] // 2
    cq = ctn // nf
    fq = ftn // nf
    scale = PERIOD // (2 * FC)

    def source(p):
        step = (nb - (p + 1) // 2) if p % 2 else p // 2
        return lax.rem(me + step, nb)

    def other(k):
        return lax.rem(fx + k, nf)

    right = lax.rem(me + 1, nb)
    left = lax.rem(me + nb - 1, nb)

    def c_move(p):
        return pltpu.make_async_remote_copy(
            src_ref=cbuf.at[max(p - 2, 0)],
            dst_ref=cbuf.at[p],
            send_sem=c_send.at[p],
            recv_sem=c_recv.at[p],
            device_id={"bank": right if p % 2 else left},
            device_id_type=MESH,
        )

    def f_move(p, c, leftward=None):
        if leftward is None:
            leftward = p % 2 == 0
        origin = p - 1 if (p == nb - 1 and leftward) else max(p - 2, 0)
        part = pl.ds(pl.multiple_of(c * fpart, fpart), fpart)
        return pltpu.make_async_remote_copy(
            src_ref=fbuf.at[origin, :, part],
            dst_ref=fbuf.at[p, :, part],
            send_sem=f_send.at[p, c],
            recv_sem=f_recv.at[p, c],
            device_id={"bank": left if leftward else right},
            device_id_type=MESH,
        )

    def n_move(k):
        return pltpu.make_async_remote_copy(
            src_ref=nstage.at[other(k)],
            dst_ref=nrecv.at[k - 1],
            send_sem=n_send.at[k - 1],
            recv_sem=n_recv.at[k - 1],
            device_id={"freq": other(k)},
            device_id_type=MESH,
        )

    def cx_move(g, k):
        return pltpu.make_async_remote_copy(
            src_ref=cstage.at[g, other(k)],
            dst_ref=crecv.at[g, k - 1],
            send_sem=cx_send.at[g, k - 1],
            recv_sem=cx_recv.at[g, k - 1],
            device_id={"freq": other(k)},
            device_id_type=MESH,
        )

    def fx_move(g, k):
        return pltpu.make_async_remote_copy(
            src_ref=fstage.at[g, other(k)],
            dst_ref=frecv.at[g, k - 1],
            send_sem=fx_send.at[g, k - 1],
            recv_sem=fx_recv.at[g, k - 1],
            device_id={"freq": other(k)},
            device_id_type=MESH,
        )

    def r_move(p):
        return pltpu.make_async_remote_copy(
            src_ref=rstage.at[p // 4 if p < nb - 1 else groups],
            dst_ref=rrecv.at[p],
            send_sem=r_send.at[p],
            recv_sem=r_recv.at[p],
            device_id={"bank": source(p)},
            device_id_type=MESH,
        )

    own_c = pltpu.make_async_copy(cs_hbm, craw, load_sem.at[0])
    own_f = pltpu.make_async_copy(fs_hbm, fraw, load_sem.at[1])
    own_c.start()
    own_f.start()
    load_cw = pltpu.make_async_copy(cw_hbm, cw, w_sem.at[0])
    load_fw = pltpu.make_async_copy(fw_hbm, fw, w_sem.at[1])
    load_cw.start()
    load_fw.start()
    load_ct = pltpu.make_async_copy(ct_hbm, ct, ct_sem)
    load_ft = pltpu.make_async_copy(ft_hbm, ft, ft_sem)

    barrier = pltpu.get_barrier_semaphore()
    for neighbour in (left, right):
        pl.semaphore_signal(barrier, inc=1, device_id={"bank": neighbour}, device_id_type=MESH)
    for k in range(1, nf):
        pl.semaphore_signal(barrier, inc=1, device_id={"freq": other(k)}, device_id_type=MESH)
    own_c.wait()
    own_f.wait()
    load_ct.start()
    load_ft.start()

    def settle(raw, buf, begin, size):
        for at in range(begin, begin + size, STEP):
            piece = [raw[r, :, at : at + STEP].astype(jnp.float32) for r in range(segs)]
            buf[0, :, at : at + STEP] = jnp.concatenate(piece, axis=0).astype(jnp.bfloat16)

    settle(fraw, fbuf, 0, fpart)
    pl.semaphore_wait(barrier, 2 + nf - 1)
    for c in range(parts):
        if c + 1 < parts:
            settle(fraw, fbuf, (c + 1) * fpart, fpart)
        else:
            settle(craw, cbuf, 0, cbins)
        for p in (1, 2):
            f_move(p, c).start()
    for p in (1, 2):
        c_move(p).start()
    load_cw.wait()
    load_fw.wait()

    def c_phases(i, carry):
        at = pl.ds(pl.multiple_of(i * STEP, STEP), STEP)
        lag = lax.broadcasted_iota(jnp.int32, (LC, STEP), 0) * CSTRIDE
        f = fx * cbins + i * STEP + lax.broadcasted_iota(jnp.int32, (LC, STEP), 1)
        cos, sin = unit_phase((f * lag * scale) & (PERIOD - 1))
        w = cw[:, at]
        ctab[0, :, at] = cos * w
        ctab[1, :, at] = sin * w
        return carry

    lax.fori_loop(0, cbins // STEP, c_phases, 0)

    def f_phases(i, carry):
        at = pl.ds(pl.multiple_of(i * STEP, STEP), STEP)
        lag = lax.broadcasted_iota(jnp.int32, (LF, STEP), 0)
        f = fx * fbins + i * STEP + lax.broadcasted_iota(jnp.int32, (LF, STEP), 1)
        cos, sin = unit_phase((f * lag) & (PERIOD - 1))
        w = fw[:, at]
        ftab[0, :, at] = cos * w
        ftab[1, :, at] = sin * w
        return carry

    lax.fori_loop(0, fbins // STEP, f_phases, 0)

    rows = lax.broadcasted_iota(jnp.int32, (16, 8 * segs), 0)
    cols = lax.broadcasted_iota(jnp.int32, (16, 8 * segs), 1)
    orow = lax.broadcasted_iota(jnp.int32, (8, LANES), 0)
    units = [list(range(4 * g, min(4 * g + 4, nb - 1))) for g in range(groups)] + [[nb - 1]]
    for u, places in enumerate(units):
        pick = jnp.zeros((16, 8 * segs), jnp.float32)
        shift = jnp.zeros((8, LANES), jnp.int32)
        for i, p in enumerate(places):
            base = source(p) * segs
            found = jnp.int32(0)
            for s in range(segs):
                for k in range(2):
                    hit = jnp.where(trig[k, base + s] == me, 1, 0)
                    slot = 2 * i + found
                    row = (rows & 7) >> 2 if u == groups else rows & 7
                    col = (i * segs + s) * 2
                    here = (row == slot) & (cols == col + (rows >> 3))
                    pick += jnp.where(here, hit.astype(jnp.float32), 0.0)
                    shift += jnp.where((orow >> 2 if u == groups else orow) == slot, hit * offs[k, base + s], 0)
                    found = found + hit
        sel[u] = pick.astype(jnp.bfloat16)
        soff[u] = shift

    def powers():
        load_ct.wait()

        def c_power(i, total):
            at = pl.ds(pl.multiple_of(i * LANES, LANES), LANES)
            re = ct[:ctn, at].astype(jnp.float32)
            im = ct[ctn:, at].astype(jnp.float32)
            return total + (re * re + im * im) * cw[:, at]

        ct_sum = lax.fori_loop(0, cbins // LANES, c_power, jnp.zeros((ctn, LANES), jnp.float32), unroll=2)
        ct_sum = jnp.broadcast_to(jnp.sum(ct_sum, axis=1, keepdims=True), (ctn, LANES))
        load_ft.wait()

        def f_power(i, total):
            at = pl.ds(pl.multiple_of(i * LANES, LANES), LANES)
            re = ft[:ftn, at].astype(jnp.float32)
            im = ft[ftn:, at].astype(jnp.float32)
            return total + (re * re + im * im) * fw[:, at]

        ft_sum = lax.fori_loop(0, fbins // LANES, f_power, jnp.zeros((ftn, LANES), jnp.float32), unroll=4)
        ft_sum = jnp.broadcast_to(jnp.sum(ft_sum, axis=1, keepdims=True), (ftn, LANES))
        for q in range(nf):
            nstage[q, :cq] = ct_sum[q * cq : (q + 1) * cq]
            nstage[q, cq:] = ft_sum[q * fq : (q + 1) * fq]

    def coarse_group(g):
        half = 4 * segs
        prow = lax.broadcasted_iota(jnp.int32, (2 * half, 2 * half), 0)
        pcol = lax.broadcasted_iota(jnp.int32, (2 * half, 2 * half), 1)
        want = jnp.where(prow < half, 2 * prow, 2 * (prow - half) + 1)
        split = jnp.where(pcol == want, 1.0, 0.0).astype(jnp.bfloat16)
        ncol = LC * half
        wide = min(2 * STEP, cbins)
        for begin in range(0, cbins, wide):
            at = slice(begin, begin + wide)
            block = jnp.concatenate([cbuf[4 * g + b, :, at].astype(jnp.float32) for b in range(4)], axis=0)
            cpure[:, at] = lax.dot_general(split, block.astype(jnp.bfloat16), NN, preferred_element_type=jnp.float32)
        cpq[...] = jnp.zeros_like(cpq)
        deep = min(DEEP, cbins)

        def step(i, carry):
            base = pl.multiple_of(i * deep, deep)
            for kt in range(0, deep, 2 * LANES):
                at = pl.ds(base + kt, 2 * LANES)
                yr, yi = cpure[:half, at], cpure[half:, at]
                for j in range(LC):
                    c = ctab[0, j : j + 1, at]
                    s = ctab[1, j : j + 1, at]
                    clag[j * half : (j + 1) * half, kt : kt + 2 * LANES] = (yr * c - yi * s).astype(jnp.bfloat16)
                    clag[ncol + j * half : ncol + (j + 1) * half, kt : kt + 2 * LANES] = (yr * s + yi * c).astype(jnp.bfloat16)
            cpq[...] += lax.dot_general(clag[...], ct[:, pl.ds(base, deep)], NT, preferred_element_type=jnp.float32)
            return carry

        lax.fori_loop(0, cbins // deep, step, 0)
        re = (cpq[:ncol, :ctn] + cpq[ncol:, ctn:]).T
        im = (cpq[ncol:, :ctn] - cpq[:ncol, ctn:]).T
        for q in range(nf):
            cstage[g, q, :cq] = re[q * cq : (q + 1) * cq]
            cstage[g, q, cq:] = im[q * cq : (q + 1) * cq]

    def fine_piece(u, c):
        single = u == groups
        ncol = LF * (2 if single else 8)
        low = lax.broadcasted_iota(jnp.int32, (8, 2 * LANES), 0) < 4
        places = units[u] + (units[groups - 1] if single else [])
        places = (places + places)[:4]
        wide = min(2 * STEP, fpart)
        for begin in range(0, fpart, wide):
            first = c * fpart + begin
            at = pl.ds(pl.multiple_of(first, wide), wide)
            block = jnp.concatenate([fbuf[p, :, at].astype(jnp.float32) for p in places], axis=0)
            y = lax.dot_general(sel[u], block.astype(jnp.bfloat16), NN, preferred_element_type=jnp.float32)
            f = fx * fbins + first + lax.broadcasted_iota(jnp.int32, (8, wide), 1)
            shift = jnp.concatenate([soff[u]] * (wide // LANES), axis=1)
            cos, sin = unit_phase((f * shift) & (PERIOD - 1))
            yr, yi = y[:8], y[8:]
            fpure[:8, begin : begin + wide] = yr * cos - yi * sin
            fpure[8:, begin : begin + wide] = yr * sin + yi * cos
        deep = min(DEEP, fpart)

        def step(i, carry):
            base = pl.multiple_of(i * deep, deep)
            whole = pl.multiple_of(c * fpart + i * deep, deep)
            for kt in range(0, deep, 2 * LANES):
                sr = fpure[:8, pl.ds(base + kt, 2 * LANES)]
                si = fpure[8:, pl.ds(base + kt, 2 * LANES)]
                at = pl.ds(whole + kt, 2 * LANES)
                here = slice(kt, kt + 2 * LANES)
                for j in range(0, ncol // 8, 2):
                    if single:
                        pair = []
                        for part in range(2):
                            rows8 = ftab[part, j * 4 : j * 4 + 8, at]
                            turned = pltpu.roll(rows8, 4, 0)
                            pair.append((jnp.where(low, rows8, turned), jnp.where(low, turned, rows8)))
                    res, ims = [], []
                    for jj in range(2):
                        if single:
                            wc, ws = pair[0][jj], pair[1][jj]
                        else:
                            wc = ftab[0, j + jj : j + jj + 1, at]
                            ws = ftab[1, j + jj : j + jj + 1, at]
                        res.append(sr * wc - si * ws)
                        ims.append(sr * ws + si * wc)
                    flag[j * 8 : j * 8 + 16, here] = jnp.concatenate(res, axis=0).astype(jnp.bfloat16)
                    flag[ncol + j * 8 : ncol + j * 8 + 16, here] = jnp.concatenate(ims, axis=0).astype(jnp.bfloat16)
            fpq[: 2 * ncol] += lax.dot_general(
                flag[: 2 * ncol], ft[:, pl.ds(whole, deep)], NT, preferred_element_type=jnp.float32
            )
            return carry

        lax.fori_loop(0, fpart // deep, step, 0)

    def fine_done(u):
        ncol = LF * (2 if u == groups else 8)
        top, bottom = fpq[:ncol], fpq[ncol : 2 * ncol]
        re = top + pltpu.roll(bottom, ftn, 1)
        im = bottom - pltpu.roll(top, ftn, 1)
        if ncol < LANES:
            rest = jnp.zeros((LANES - ncol, LANES), jnp.float32)
            re = jnp.concatenate([re, rest], axis=0)
            im = jnp.concatenate([im, rest], axis=0)
        re, im = re.T, im.T
        for q in range(nf):
            fstage[u, q, :fq] = re[q * fq : (q + 1) * fq]
            fstage[u, q, fq:] = im[q * fq : (q + 1) * fq]

    def coarse_peak(g):
        total = cstage[g, fx]
        for k in range(1, nf):
            cx_move(g, k).wait_recv()
            total = total + crecv[g, k - 1]
        energy = total[:cq] * total[:cq] + total[cq:] * total[cq:]
        half = 4 * segs
        peak = energy[:, :LANES]
        for b in range(1, LC * half // LANES):
            peak = jnp.maximum(peak, energy[:, b * LANES : (b + 1) * LANES])
        span = LANES // 2
        while span >= half:
            peak = jnp.maximum(peak, pltpu.roll(peak, span, 1))
            span //= 2
        peak = peak / cnorm[...]
        lane = lax.broadcasted_iota(jnp.int32, (cq, LANES), 1) // segs
        for i in range(4):
            src = source(4 * g + i)
            moved = pltpu.roll(peak, lax.rem(src * segs + LANES - i * segs, LANES), 1)
            cres[...] = jnp.where(lane == src, moved, cres[...])

    def fine_peak(g):
        total = fstage[g, fx]
        for k in range(1, nf):
            fx_move(g, k).wait_recv()
            total = total + frecv[g, k - 1]
        energy = total[:fq] * total[:fq] + total[fq:] * total[fq:]
        peak = energy
        for span in (16, 8, 2, 1) if g == groups else (64, 32, 16, 8):
            peak = jnp.maximum(peak, pltpu.roll(peak, LANES - span, 1))
        peak = peak / fnorm[...]
        square = jnp.concatenate([peak, jnp.zeros((LANES - fq, LANES), jnp.float32)], axis=0)
        rstage[g] = square.T[:8]

    def norms():
        total = nstage[fx]
        for k in range(1, nf):
            n_move(k).wait_recv()
            total = total + nrecv[k - 1]
        cnorm[...] = total[:cq]
        fnorm[...] = total[cq:]
        cres[...] = jnp.zeros_like(cres)

    def give_back(u):
        for p in units[u]:
            if p > 0:
                r_move(p).start()

    def start_all(move, g):
        for k in range(1, nf):
            move(g, k).start()

    def hop(h, unit=None, first=None):
        here = [p for p in (2 * h - 1, 2 * h) if p <= nb - 1]
        half = parts // 2
        if unit is not None:
            fpq[...] = jnp.zeros_like(fpq)

        def part(i, carry):
            c = (i % 2) * half + i // 2 if here == [nb - 1] else i
            for p in here:
                f_move(p, c).wait_recv()
                if p + 2 < nb - 1:
                    f_move(p + 2, c).start()
                elif p + 2 == nb - 1:

                    @pl.when(c < half)
                    def _():
                        f_move(nb - 1, c, leftward=False).start()

                elif p + 1 == nb - 1:

                    @pl.when(c >= half)
                    def _():
                        f_move(nb - 1, c, leftward=True).start()

            if first is not None:

                @pl.when(i == 0)
                def _():
                    first()

            if unit is not None:
                fine_piece(unit, c)
            return carry

        lax.fori_loop(0, parts, part, 0)
        if unit is not None:
            fine_done(unit)
            start_all(fx_move, unit)

    def pass_coarse(h):
        for p in (2 * h - 1, 2 * h):
            if p <= nb - 1:
                c_move(p).wait_recv()
                if p + 2 <= nb - 1:
                    c_move(p + 2).start()

    if groups == 1:
        powers()
        for k in range(1, nf):
            n_move(k).start()
    for g in range(groups - 1):
        hop(2 * g + 1, first=functools.partial(start_all, cx_move, g - 1) if g else None)
        pass_coarse(2 * g + 1)
        if g == 0:
            powers()
        else:
            if g == 1:
                norms()
            fine_peak(g - 1)
            give_back(g - 1)
            coarse_peak(g - 1)
        hop(2 * g + 2, g)
        pass_coarse(2 * g + 2)
        if g == 0:
            for k in range(1, nf):
                n_move(k).start()
        coarse_group(g)
    last = groups - 1
    hop(2 * last + 1, last, functools.partial(start_all, cx_move, last - 1) if last else None)
    pass_coarse(2 * last + 1)
    hop(2 * last + 2, groups)
    if groups <= 2:
        norms()
    pass_coarse(2 * last + 2)
    coarse_group(last)
    if last:
        fine_peak(last - 1)
        give_back(last - 1)
    start_all(cx_move, last)
    fine_peak(last)
    give_back(last)
    fine_peak(groups)
    give_back(groups)
    rrecv[0] = rstage[0]
    if last:
        coarse_peak(last - 1)

    spots, named = [], []
    for s in range(segs):
        for k in range(2):
            bank = trig[k, me * segs + s]
            rank = jnp.int32(0)
            for before in named:
                rank = rank + jnp.where(before == bank, 1, 0)
            named.append(bank)
            away = lax.rem(me - bank + nb, nb)
            place = jnp.where(away < nb // 2, 2 * away, 2 * (nb - away) - 1)
            row = jnp.where(place == nb - 1, 4 * rank, lax.rem(place, 4) * 2 + rank)
            spots.append((jnp.clip(place, 0, nb - 1), jnp.clip(row, 0, 7)))
    for p in range(1, nb):
        c_move(p).wait_send()
        for c in range(parts):
            f_move(p, c).wait_send()
    for k in range(1, nf):
        n_move(k).wait_send()
        for g in range(groups + 1):
            fx_move(g, k).wait_send()
            if g < last:
                cx_move(g, k).wait_send()
    for p in range(1, nb - 4):
        r_move(p).wait_send()
    coarse_peak(last)
    coarse_out[...] = cres[...]
    for k in range(1, nf):
        cx_move(last, k).wait_send()
    for p in range(max(1, nb - 4), nb):
        r_move(p).wait_send()
    for p in range(1, nb):
        r_move(p).wait_recv()
    result = jnp.zeros((8, LANES), jnp.float32)
    for n, (place, row) in enumerate(spots):
        line = rrecv[place, pl.ds(row, 1), :]
        result = jnp.where(orow == n, line, result)
    fine_out[...] = result


def body(
    nb,
    nf,
    coarse_spectra,
    fine_spectra,
    coarse_templates,
    fine_templates,
    coarse_weight,
    fine_weight,
    triggers,
    offsets,
):
    segs, _, cbins = coarse_spectra.shape
    fbins = fine_spectra.shape[2]
    ctn = coarse_templates.shape[1]
    ftn = fine_templates.shape[2]
    groups = nb // 4
    parts = 4
    cq, fq = ctn // nf, ftn // nf
    ccol, fcol = LC * 4 * segs, LF * 8
    f32, bf16 = jnp.float32, jnp.bfloat16
    dma = pltpu.SemaphoreType.DMA
    anywhere = pl.BlockSpec(memory_space=pl.ANY)
    smem = pl.BlockSpec(memory_space=pltpu.SMEM)
    vmem = pl.BlockSpec(memory_space=pltpu.VMEM)
    coarse, fine = pl.pallas_call(
        functools.partial(kernel, nb, nf),
        out_shape=(
            jax.ShapeDtypeStruct((cq, LANES), f32),
            jax.ShapeDtypeStruct((8, LANES), f32),
        ),
        in_specs=[smem, smem] + [anywhere] * 6,
        out_specs=(vmem, vmem),
        scratch_shapes=[
            pltpu.VMEM((segs, 2, cbins), bf16),
            pltpu.VMEM((segs, 2, fbins), bf16),
            pltpu.VMEM((nb, 2 * segs, cbins), bf16),
            pltpu.VMEM((nb, 2 * segs, fbins), bf16),
            pltpu.VMEM((2 * ctn, cbins), bf16),
            pltpu.VMEM((2 * ftn, fbins), bf16),
            pltpu.VMEM((1, cbins), f32),
            pltpu.VMEM((1, fbins), f32),
            pltpu.VMEM((8 * segs, cbins), f32),
            pltpu.VMEM((16, fbins // parts), f32),
            pltpu.VMEM((2, LC, cbins), f32),
            pltpu.VMEM((2, LF, fbins), f32),
            pltpu.VMEM((2 * ccol, min(DEEP, cbins)), bf16),
            pltpu.VMEM((2 * fcol, min(DEEP, fbins // parts)), bf16),
            pltpu.VMEM((2 * ccol, 2 * ctn), f32),
            pltpu.VMEM((2 * fcol, 2 * ftn), f32),
            pltpu.VMEM((groups + 1, 16, 8 * segs), bf16),
            pltpu.VMEM((groups + 1, 8, LANES), jnp.int32),
            pltpu.VMEM((groups, nf, 2 * cq, ccol), f32),
            pltpu.VMEM((groups, nf - 1, 2 * cq, ccol), f32),
            pltpu.VMEM((groups + 1, nf, 2 * fq, fcol), f32),
            pltpu.VMEM((groups + 1, nf - 1, 2 * fq, fcol), f32),
            pltpu.VMEM((nf, cq + fq, LANES), f32),
            pltpu.VMEM((nf - 1, cq + fq, LANES), f32),
            pltpu.VMEM((cq, LANES), f32),
            pltpu.VMEM((fq, LANES), f32),
            pltpu.VMEM((cq, LANES), f32),
            pltpu.VMEM((groups + 1, 8, LANES), f32),
            pltpu.VMEM((nb, 8, LANES), f32),
            dma((2,)),
            dma((2,)),
            dma,
            dma,
            dma((nb,)),
            dma((nb,)),
            dma((nb, parts)),
            dma((nb, parts)),
            dma((nf - 1,)),
            dma((nf - 1,)),
            dma((groups, nf - 1)),
            dma((groups, nf - 1)),
            dma((groups + 1, nf - 1)),
            dma((groups + 1, nf - 1)),
            dma((nb,)),
            dma((nb,)),
        ],
        compiler_params=pltpu.CompilerParams(
            collective_id=0, has_side_effects=True, vmem_limit_bytes=67043328
        ),
        name="search",
    )(
        triggers.T,
        offsets.T,
        coarse_spectra,
        fine_spectra,
        coarse_templates.reshape(2 * ctn, cbins),
        fine_templates.reshape(2 * ftn, fbins),
        coarse_weight.reshape(1, cbins),
        fine_weight.reshape(1, fbins),
    )
    coarse_snr = coarse[:, : nb * segs]
    fine_snr = fine[:, :fq].reshape(segs, 2, fq)
    return coarse_snr, fine_snr


def solution(mesh):
    return jax.shard_map(
        functools.partial(body, mesh.shape["bank"], mesh.shape["freq"]),
        mesh=mesh,
        in_specs=(
            P(("groups", "seg", "bank"), None, "freq"),
            P(("groups", "seg", "bank"), None, "freq"),
            P(None, "bank", "freq"),
            P(None, "bank", None, "freq"),
            P(("groups", "freq")),
            P(("groups", "freq")),
            P(("groups", "seg"), None),
            P(("groups", "seg"), None),
        ),
        out_specs=(
            P(("bank", "freq"), ("groups", "seg")),
            P(("groups", "seg", "bank"), None, "freq"),
        ),
        check_vma=False,
    )
```

```python
import functools
import math

import jax
import jax.numpy as jnp
from jax import lax
from jax.experimental import pallas as pl
from jax.experimental.pallas import tpu as pltpu
from jax.sharding import PartitionSpec as P

FC = 16384
FB = 65536
CAP = 2
LC = 16
LF = 16
CSTRIDE = 2047
PERIOD = 131072
STEP = 512
DEEP = 2048
LANES = 128
MESH = pl.DeviceIdType.MESH
NT = (((1,), (1,)), ((), ()))
NN = (((1,), (0,)), ((), ()))


def unit_phase(count):
    quadrant = (count + PERIOD // 8) >> 15
    x = (count - (quadrant << 15)).astype(jnp.float32) * (2.0 * math.pi / PERIOD)
    z = x * x
    s = x * (1.0 + z * (-1.0 / 6 + z * (1.0 / 120 + z * (-1.0 / 5040 + z * (1.0 / 362880)))))
    c = 1.0 + z * (-0.5 + z * (1.0 / 24 + z * (-1.0 / 720 + z * (1.0 / 40320 - z * (1.0 / 3628800)))))
    odd = (quadrant & 1) == 1
    cos = jnp.where(odd, s, c)
    sin = jnp.where(odd, c, s)
    cos = jnp.where(((quadrant + 1) & 2) == 2, -cos, cos)
    sin = jnp.where((quadrant & 2) == 2, -sin, sin)
    return cos, sin


def kernel(
    nb,
    nf,
    trig,
    offs,
    cs_hbm,
    fs_hbm,
    ct_hbm,
    ft_hbm,
    cw_hbm,
    fw_hbm,
    coarse_out,
    fine_out,
    craw,
    fraw,
    cbuf,
    fbuf,
    ct,
    ft,
    cw,
    fw,
    cpure,
    fpure,
    ctab,
    ftab,
    clag,
    flag,
    cpq,
    fpq,
    sel,
    soff,
    cstage,
    crecv,
    fstage,
    frecv,
    nstage,
    nrecv,
    cnorm,
    fnorm,
    cres,
    rstage,
    rrecv,
    load_sem,
    w_sem,
    ct_sem,
    ft_sem,
    c_send,
    c_recv,
    f_send,
    f_recv,
    n_send,
    n_recv,
    cx_send,
    cx_recv,
    fx_send,
    fx_recv,
    r_send,
    r_recv,
):
    me = lax.axis_index("bank")
    fx = lax.axis_index("freq")
    groups = nb // 4
    segs = cbuf.shape[1] // 2
    cbins = cbuf.shape[2]
    fbins = fbuf.shape[2]
    parts = f_send.shape[1]
    fpart = fbins // parts
    ctn = ct.shape[0] // 2
    ftn = ft.shape[0] // 2
    cq = ctn // nf
    fq = ftn // nf
    scale = PERIOD // (2 * FC)

    def source(p):
        step = (nb - (p + 1) // 2) if p % 2 else p // 2
        return lax.rem(me + step, nb)

    def other(k):
        return lax.rem(fx + k, nf)

    right = lax.rem(me + 1, nb)
    left = lax.rem(me + nb - 1, nb)

    def c_move(p):
        return pltpu.make_async_remote_copy(
            src_ref=cbuf.at[max(p - 2, 0)],
            dst_ref=cbuf.at[p],
            send_sem=c_send.at[p],
            recv_sem=c_recv.at[p],
            device_id={"bank": right if p % 2 else left},
            device_id_type=MESH,
        )

    def f_move(p, c, leftward=None):
        if leftward is None:
            leftward = p % 2 == 0
        origin = p - 1 if (p == nb - 1 and leftward) else max(p - 2, 0)
        part = pl.ds(pl.multiple_of(c * fpart, fpart), fpart)
        return pltpu.make_async_remote_copy(
            src_ref=fbuf.at[origin, :, part],
            dst_ref=fbuf.at[p, :, part],
            send_sem=f_send.at[p, c],
            recv_sem=f_recv.at[p, c],
            device_id={"bank": left if leftward else right},
            device_id_type=MESH,
        )

    def n_move(k):
        return pltpu.make_async_remote_copy(
            src_ref=nstage.at[other(k)],
            dst_ref=nrecv.at[k - 1],
            send_sem=n_send.at[k - 1],
            recv_sem=n_recv.at[k - 1],
            device_id={"freq": other(k)},
            device_id_type=MESH,
        )

    def cx_move(g, k):
        return pltpu.make_async_remote_copy(
            src_ref=cstage.at[g, other(k)],
            dst_ref=crecv.at[g, k - 1],
            send_sem=cx_send.at[g, k - 1],
            recv_sem=cx_recv.at[g, k - 1],
            device_id={"freq": other(k)},
            device_id_type=MESH,
        )

    def fx_move(g, k):
        return pltpu.make_async_remote_copy(
            src_ref=fstage.at[g, other(k)],
            dst_ref=frecv.at[g, k - 1],
            send_sem=fx_send.at[g, k - 1],
            recv_sem=fx_recv.at[g, k - 1],
            device_id={"freq": other(k)},
            device_id_type=MESH,
        )

    def r_move(p):
        return pltpu.make_async_remote_copy(
            src_ref=rstage.at[p // 4 if p < nb - 1 else groups],
            dst_ref=rrecv.at[p],
            send_sem=r_send.at[p],
            recv_sem=r_recv.at[p],
            device_id={"bank": source(p)},
            device_id_type=MESH,
        )

    own_c = pltpu.make_async_copy(cs_hbm, craw, load_sem.at[0])
    own_f = pltpu.make_async_copy(fs_hbm, fraw, load_sem.at[1])
    own_c.start()
    own_f.start()
    load_cw = pltpu.make_async_copy(cw_hbm, cw, w_sem.at[0])
    load_fw = pltpu.make_async_copy(fw_hbm, fw, w_sem.at[1])
    load_cw.start()
    load_fw.start()
    load_ct = pltpu.make_async_copy(ct_hbm, ct, ct_sem)
    load_ft = pltpu.make_async_copy(ft_hbm, ft, ft_sem)

    barrier = pltpu.get_barrier_semaphore()
    for neighbour in (left, right):
        pl.semaphore_signal(barrier, inc=1, device_id={"bank": neighbour}, device_id_type=MESH)
    for k in range(1, nf):
        pl.semaphore_signal(barrier, inc=1, device_id={"freq": other(k)}, device_id_type=MESH)
    own_c.wait()
    own_f.wait()
    load_ct.start()
    load_ft.start()

    def settle(raw, buf, begin, size):
        for at in range(begin, begin + size, STEP):
            piece = [raw[r, :, at : at + STEP].astype(jnp.float32) for r in range(segs)]
            buf[0, :, at : at + STEP] = jnp.concatenate(piece, axis=0).astype(jnp.bfloat16)

    settle(fraw, fbuf, 0, fpart)
    pl.semaphore_wait(barrier, 2 + nf - 1)
    for c in range(parts):
        if c + 1 < parts:
            settle(fraw, fbuf, (c + 1) * fpart, fpart)
        else:
            settle(craw, cbuf, 0, cbins)
        for p in (1, 2):
            f_move(p, c).start()
    for p in (1, 2):
        c_move(p).start()
    load_cw.wait()
    load_fw.wait()

    def c_phases(i, carry):
        at = pl.ds(pl.multiple_of(i * STEP, STEP), STEP)
        lag = lax.broadcasted_iota(jnp.int32, (LC, STEP), 0) * CSTRIDE
        f = fx * cbins + i * STEP + lax.broadcasted_iota(jnp.int32, (LC, STEP), 1)
        cos, sin = unit_phase((f * lag * scale) & (PERIOD - 1))
        w = cw[:, at]
        ctab[0, :, at] = cos * w
        ctab[1, :, at] = sin * w
        return carry

    lax.fori_loop(0, cbins // STEP, c_phases, 0)

    def f_phases(i, carry):
        at = pl.ds(pl.multiple_of(i * STEP, STEP), STEP)
        lag = lax.broadcasted_iota(jnp.int32, (LF, STEP), 0)
        f = fx * fbins + i * STEP + lax.broadcasted_iota(jnp.int32, (LF, STEP), 1)
        cos, sin = unit_phase((f * lag) & (PERIOD - 1))
        w = fw[:, at]
        ftab[0, :, at] = cos * w
        ftab[1, :, at] = sin * w
        return carry

    lax.fori_loop(0, fbins // STEP, f_phases, 0)

    rows = lax.broadcasted_iota(jnp.int32, (16, 8 * segs), 0)
    cols = lax.broadcasted_iota(jnp.int32, (16, 8 * segs), 1)
    orow = lax.broadcasted_iota(jnp.int32, (8, LANES), 0)
    units = [list(range(4 * g, min(4 * g + 4, nb - 1))) for g in range(groups)] + [[nb - 1]]
    for u, places in enumerate(units):
        pick = jnp.zeros((16, 8 * segs), jnp.float32)
        shift = jnp.zeros((8, LANES), jnp.int32)
        for i, p in enumerate(places):
            base = source(p) * segs
            found = jnp.int32(0)
            for s in range(segs):
                for k in range(2):
                    hit = jnp.where(trig[k, base + s] == me, 1, 0)
                    slot = 2 * i + found
                    row = (rows & 7) >> 2 if u == groups else rows & 7
                    col = (i * segs + s) * 2
                    here = (row == slot) & (cols == col + (rows >> 3))
                    pick += jnp.where(here, hit.astype(jnp.float32), 0.0)
                    shift += jnp.where((orow >> 2 if u == groups else orow) == slot, hit * offs[k, base + s], 0)
                    found = found + hit
        sel[u] = pick.astype(jnp.bfloat16)
        soff[u] = shift

    def powers():
        load_ct.wait()

        def c_power(i, total):
            at = pl.ds(pl.multiple_of(i * LANES, LANES), LANES)
            re = ct[:ctn, at].astype(jnp.float32)
            im = ct[ctn:, at].astype(jnp.float32)
            return total + (re * re + im * im) * cw[:, at]

        ct_sum = lax.fori_loop(0, cbins // LANES, c_power, jnp.zeros((ctn, LANES), jnp.float32), unroll=2)
        ct_sum = jnp.broadcast_to(jnp.sum(ct_sum, axis=1, keepdims=True), (ctn, LANES))
        load_ft.wait()

        def f_power(i, total):
            at = pl.ds(pl.multiple_of(i * LANES, LANES), LANES)
            re = ft[:ftn, at].astype(jnp.float32)
            im = ft[ftn:, at].astype(jnp.float32)
            return total + (re * re + im * im) * fw[:, at]

        ft_sum = lax.fori_loop(0, fbins // LANES, f_power, jnp.zeros((ftn, LANES), jnp.float32), unroll=4)
        ft_sum = jnp.broadcast_to(jnp.sum(ft_sum, axis=1, keepdims=True), (ftn, LANES))
        for q in range(nf):
            nstage[q, :cq] = ct_sum[q * cq : (q + 1) * cq]
            nstage[q, cq:] = ft_sum[q * fq : (q + 1) * fq]

    def coarse_group(g):
        half = 4 * segs
        prow = lax.broadcasted_iota(jnp.int32, (2 * half, 2 * half), 0)
        pcol = lax.broadcasted_iota(jnp.int32, (2 * half, 2 * half), 1)
        want = jnp.where(prow < half, 2 * prow, 2 * (prow - half) + 1)
        split = jnp.where(pcol == want, 1.0, 0.0).astype(jnp.bfloat16)
        ncol = LC * half
        wide = min(2 * STEP, cbins)
        for begin in range(0, cbins, wide):
            at = slice(begin, begin + wide)
            block = jnp.concatenate([cbuf[4 * g + b, :, at].astype(jnp.float32) for b in range(4)], axis=0)
            cpure[:, at] = lax.dot_general(split, block.astype(jnp.bfloat16), NN, preferred_element_type=jnp.float32)
        cpq[...] = jnp.zeros_like(cpq)
        deep = min(DEEP, cbins)

        def step(i, carry):
            base = pl.multiple_of(i * deep, deep)
            for kt in range(0, deep, 2 * LANES):
                at = pl.ds(base + kt, 2 * LANES)
                yr, yi = cpure[:half, at], cpure[half:, at]
                for j in range(LC):
                    c = ctab[0, j : j + 1, at]
                    s = ctab[1, j : j + 1, at]
                    clag[j * half : (j + 1) * half, kt : kt + 2 * LANES] = (yr * c - yi * s).astype(jnp.bfloat16)
                    clag[ncol + j * half : ncol + (j + 1) * half, kt : kt + 2 * LANES] = (yr * s + yi * c).astype(jnp.bfloat16)
            cpq[...] += lax.dot_general(clag[...], ct[:, pl.ds(base, deep)], NT, preferred_element_type=jnp.float32)
            return carry

        lax.fori_loop(0, cbins // deep, step, 0)
        re = (cpq[:ncol, :ctn] + cpq[ncol:, ctn:]).T
        im = (cpq[ncol:, :ctn] - cpq[:ncol, ctn:]).T
        for q in range(nf):
            cstage[g, q, :cq] = re[q * cq : (q + 1) * cq]
            cstage[g, q, cq:] = im[q * cq : (q + 1) * cq]

    def fine_piece(u, c):
        single = u == groups
        ncol = LF * (2 if single else 8)
        low = lax.broadcasted_iota(jnp.int32, (8, 2 * LANES), 0) < 4
        places = units[u] + (units[groups - 1] if single else [])
        places = (places + places)[:4]
        wide = min(2 * STEP, fpart)
        for begin in range(0, fpart, wide):
            first = c * fpart + begin
            at = pl.ds(pl.multiple_of(first, wide), wide)
            block = jnp.concatenate([fbuf[p, :, at].astype(jnp.float32) for p in places], axis=0)
            y = lax.dot_general(sel[u], block.astype(jnp.bfloat16), NN, preferred_element_type=jnp.float32)
            f = fx * fbins + first + lax.broadcasted_iota(jnp.int32, (8, wide), 1)
            shift = jnp.concatenate([soff[u]] * (wide // LANES), axis=1)
            cos, sin = unit_phase((f * shift) & (PERIOD - 1))
            yr, yi = y[:8], y[8:]
            fpure[:8, begin : begin + wide] = yr * cos - yi * sin
            fpure[8:, begin : begin + wide] = yr * sin + yi * cos
        deep = fpart if single else min(DEEP, fpart)

        def step(i, carry):
            base = pl.multiple_of(i * deep, deep)
            whole = pl.multiple_of(c * fpart + i * deep, deep)
            for kt in range(0, deep, 2 * LANES):
                sr = fpure[:8, pl.ds(base + kt, 2 * LANES)]
                si = fpure[8:, pl.ds(base + kt, 2 * LANES)]
                at = pl.ds(whole + kt, 2 * LANES)
                here = slice(kt, kt + 2 * LANES)
                for j in range(0, ncol // 8, 2):
                    if single:
                        pair = []
                        for part in range(2):
                            rows8 = ftab[part, j * 4 : j * 4 + 8, at]
                            turned = pltpu.roll(rows8, 4, 0)
                            pair.append((jnp.where(low, rows8, turned), jnp.where(low, turned, rows8)))
                    res, ims = [], []
                    for jj in range(2):
                        if single:
                            wc, ws = pair[0][jj], pair[1][jj]
                        else:
                            wc = ftab[0, j + jj : j + jj + 1, at]
                            ws = ftab[1, j + jj : j + jj + 1, at]
                        res.append(sr * wc - si * ws)
                        ims.append(sr * ws + si * wc)
                    flag[j * 8 : j * 8 + 16, here] = jnp.concatenate(res, axis=0).astype(jnp.bfloat16)
                    flag[ncol + j * 8 : ncol + j * 8 + 16, here] = jnp.concatenate(ims, axis=0).astype(jnp.bfloat16)
            fpq[: 2 * ncol] += lax.dot_general(
                flag[: 2 * ncol, :deep], ft[:, pl.ds(whole, deep)], NT, preferred_element_type=jnp.float32
            )
            return carry

        lax.fori_loop(0, fpart // deep, step, 0)

    def fine_done(u):
        ncol = LF * (2 if u == groups else 8)
        top, bottom = fpq[:ncol], fpq[ncol : 2 * ncol]
        re = top + pltpu.roll(bottom, ftn, 1)
        im = bottom - pltpu.roll(top, ftn, 1)
        if ncol < LANES:
            rest = jnp.zeros((LANES - ncol, LANES), jnp.float32)
            re = jnp.concatenate([re, rest], axis=0)
            im = jnp.concatenate([im, rest], axis=0)
        re, im = re.T, im.T
        for q in range(nf):
            fstage[u, q, :fq] = re[q * fq : (q + 1) * fq]
            fstage[u, q, fq:] = im[q * fq : (q + 1) * fq]

    def coarse_peak(g):
        total = cstage[g, fx]
        for k in range(1, nf):
            cx_move(g, k).wait_recv()
            total = total + crecv[g, k - 1]
        energy = total[:cq] * total[:cq] + total[cq:] * total[cq:]
        half = 4 * segs
        peak = energy[:, :LANES]
        for b in range(1, LC * half // LANES):
            peak = jnp.maximum(peak, energy[:, b * LANES : (b + 1) * LANES])
        span = LANES // 2
        while span >= half:
            peak = jnp.maximum(peak, pltpu.roll(peak, span, 1))
            span //= 2
        peak = peak / cnorm[...]
        lane = lax.broadcasted_iota(jnp.int32, (cq, LANES), 1) // segs
        for i in range(4):
            src = source(4 * g + i)
            moved = pltpu.roll(peak, lax.rem(src * segs + LANES - i * segs, LANES), 1)
            cres[...] = jnp.where(lane == src, moved, cres[...])

    def fine_peak(g):
        total = fstage[g, fx]
        for k in range(1, nf):
            fx_move(g, k).wait_recv()
            total = total + frecv[g, k - 1]
        energy = total[:fq] * total[:fq] + total[fq:] * total[fq:]
        peak = energy
        for span in (16, 8, 2, 1) if g == groups else (64, 32, 16, 8):
            peak = jnp.maximum(peak, pltpu.roll(peak, LANES - span, 1))
        peak = peak / fnorm[...]
        square = jnp.concatenate([peak, jnp.zeros((LANES - fq, LANES), jnp.float32)], axis=0)
        rstage[g] = square.T[:8]

    def norms():
        total = nstage[fx]
        for k in range(1, nf):
            n_move(k).wait_recv()
            total = total + nrecv[k - 1]
        cnorm[...] = total[:cq]
        fnorm[...] = total[cq:]
        cres[...] = jnp.zeros_like(cres)

    def give_back(u):
        for p in units[u]:
            if p > 0:
                r_move(p).start()

    def start_all(move, g):
        for k in range(1, nf):
            move(g, k).start()

    def hop(h, unit=None, first=None):
        here = [p for p in (2 * h - 1, 2 * h) if p <= nb - 1]
        half = parts // 2
        if unit is not None:
            fpq[...] = jnp.zeros_like(fpq)

        def part(i, carry):
            c = (i % 2) * half + i // 2 if here == [nb - 1] else i
            for p in here:
                f_move(p, c).wait_recv()
                if p + 2 < nb - 1:
                    f_move(p + 2, c).start()
                elif p + 2 == nb - 1:

                    @pl.when(c < half)
                    def _():
                        f_move(nb - 1, c, leftward=False).start()

                elif p + 1 == nb - 1:

                    @pl.when(c >= half)
                    def _():
                        f_move(nb - 1, c, leftward=True).start()

            if first is not None:

                @pl.when(i == 0)
                def _():
                    first()

            if unit is not None:
                fine_piece(unit, c)
            return carry

        lax.fori_loop(0, parts, part, 0)
        if unit is not None:
            fine_done(unit)
            start_all(fx_move, unit)

    def pass_coarse(h):
        for p in (2 * h - 1, 2 * h):
            if p <= nb - 1:
                c_move(p).wait_recv()
                if p + 2 <= nb - 1:
                    c_move(p + 2).start()

    if groups == 1:
        powers()
        for k in range(1, nf):
            n_move(k).start()
    for g in range(groups - 1):
        hop(2 * g + 1, first=functools.partial(start_all, cx_move, g - 1) if g else None)
        pass_coarse(2 * g + 1)
        if g == 0:
            powers()
        else:
            if g == 1:
                norms()
            fine_peak(g - 1)
            give_back(g - 1)
            coarse_peak(g - 1)
        hop(2 * g + 2, g)
        pass_coarse(2 * g + 2)
        if g == 0:
            for k in range(1, nf):
                n_move(k).start()
        coarse_group(g)
    last = groups - 1
    hop(2 * last + 1, last, functools.partial(start_all, cx_move, last - 1) if last else None)
    pass_coarse(2 * last + 1)
    hop(2 * last + 2, groups)
    if groups <= 2:
        norms()
    pass_coarse(2 * last + 2)
    coarse_group(last)
    start_all(cx_move, last)
    if last:
        fine_peak(last - 1)
        give_back(last - 1)
    fine_peak(last)
    give_back(last)
    fine_peak(groups)
    give_back(groups)
    rrecv[0] = rstage[0]
    if last:
        coarse_peak(last - 1)

    spots, named = [], []
    for s in range(segs):
        for k in range(2):
            bank = trig[k, me * segs + s]
            rank = jnp.int32(0)
            for before in named:
                rank = rank + jnp.where(before == bank, 1, 0)
            named.append(bank)
            away = lax.rem(me - bank + nb, nb)
            place = jnp.where(away < nb // 2, 2 * away, 2 * (nb - away) - 1)
            row = jnp.where(place == nb - 1, 4 * rank, lax.rem(place, 4) * 2 + rank)
            spots.append((jnp.clip(place, 0, nb - 1), jnp.clip(row, 0, 7)))
    for p in range(1, nb):
        c_move(p).wait_send()
        for c in range(parts):
            f_move(p, c).wait_send()
    for k in range(1, nf):
        n_move(k).wait_send()
        for g in range(groups + 1):
            fx_move(g, k).wait_send()
            if g < last:
                cx_move(g, k).wait_send()
    for p in range(1, nb - 4):
        r_move(p).wait_send()
    coarse_peak(last)
    coarse_out[...] = cres[...]
    for k in range(1, nf):
        cx_move(last, k).wait_send()
    for p in range(max(1, nb - 4), nb):
        r_move(p).wait_send()
    for p in range(1, nb):
        r_move(p).wait_recv()
    result = jnp.zeros((8, LANES), jnp.float32)
    for n, (place, row) in enumerate(spots):
        line = rrecv[place, pl.ds(row, 1), :]
        result = jnp.where(orow == n, line, result)
    fine_out[...] = result


def body(
    nb,
    nf,
    coarse_spectra,
    fine_spectra,
    coarse_templates,
    fine_templates,
    coarse_weight,
    fine_weight,
    triggers,
    offsets,
):
    segs, _, cbins = coarse_spectra.shape
    fbins = fine_spectra.shape[2]
    ctn = coarse_templates.shape[1]
    ftn = fine_templates.shape[2]
    groups = nb // 4
    parts = 4
    cq, fq = ctn // nf, ftn // nf
    ccol, fcol = LC * 4 * segs, LF * 8
    f32, bf16 = jnp.float32, jnp.bfloat16
    dma = pltpu.SemaphoreType.DMA
    anywhere = pl.BlockSpec(memory_space=pl.ANY)
    smem = pl.BlockSpec(memory_space=pltpu.SMEM)
    vmem = pl.BlockSpec(memory_space=pltpu.VMEM)
    coarse, fine = pl.pallas_call(
        functools.partial(kernel, nb, nf),
        out_shape=(
            jax.ShapeDtypeStruct((cq, LANES), f32),
            jax.ShapeDtypeStruct((8, LANES), f32),
        ),
        in_specs=[smem, smem] + [anywhere] * 6,
        out_specs=(vmem, vmem),
        scratch_shapes=[
            pltpu.VMEM((segs, 2, cbins), bf16),
            pltpu.VMEM((segs, 2, fbins), bf16),
            pltpu.VMEM((nb, 2 * segs, cbins), bf16),
            pltpu.VMEM((nb, 2 * segs, fbins), bf16),
            pltpu.VMEM((2 * ctn, cbins), bf16),
            pltpu.VMEM((2 * ftn, fbins), bf16),
            pltpu.VMEM((1, cbins), f32),
            pltpu.VMEM((1, fbins), f32),
            pltpu.VMEM((8 * segs, cbins), f32),
            pltpu.VMEM((16, fbins // parts), f32),
            pltpu.VMEM((2, LC, cbins), f32),
            pltpu.VMEM((2, LF, fbins), f32),
            pltpu.VMEM((2 * ccol, min(DEEP, cbins)), bf16),
            pltpu.VMEM((2 * fcol, fbins // parts), bf16),
            pltpu.VMEM((2 * ccol, 2 * ctn), f32),
            pltpu.VMEM((2 * fcol, 2 * ftn), f32),
            pltpu.VMEM((groups + 1, 16, 8 * segs), bf16),
            pltpu.VMEM((groups + 1, 8, LANES), jnp.int32),
            pltpu.VMEM((groups, nf, 2 * cq, ccol), f32),
            pltpu.VMEM((groups, nf - 1, 2 * cq, ccol), f32),
            pltpu.VMEM((groups + 1, nf, 2 * fq, fcol), f32),
            pltpu.VMEM((groups + 1, nf - 1, 2 * fq, fcol), f32),
            pltpu.VMEM((nf, cq + fq, LANES), f32),
            pltpu.VMEM((nf - 1, cq + fq, LANES), f32),
            pltpu.VMEM((cq, LANES), f32),
            pltpu.VMEM((fq, LANES), f32),
            pltpu.VMEM((cq, LANES), f32),
            pltpu.VMEM((groups + 1, 8, LANES), f32),
            pltpu.VMEM((nb, 8, LANES), f32),
            dma((2,)),
            dma((2,)),
            dma,
            dma,
            dma((nb,)),
            dma((nb,)),
            dma((nb, parts)),
            dma((nb, parts)),
            dma((nf - 1,)),
            dma((nf - 1,)),
            dma((groups, nf - 1)),
            dma((groups, nf - 1)),
            dma((groups + 1, nf - 1)),
            dma((groups + 1, nf - 1)),
            dma((nb,)),
            dma((nb,)),
        ],
        compiler_params=pltpu.CompilerParams(
            collective_id=0, has_side_effects=True, vmem_limit_bytes=55200 * 1024
        ),
        name="search",
    )(
        triggers.T,
        offsets.T,
        coarse_spectra,
        fine_spectra,
        coarse_templates.reshape(2 * ctn, cbins),
        fine_templates.reshape(2 * ftn, fbins),
        coarse_weight.reshape(1, cbins),
        fine_weight.reshape(1, fbins),
    )
    coarse_snr = coarse[:, : nb * segs]
    fine_snr = fine[:, :fq].reshape(segs, 2, fq)
    return coarse_snr, fine_snr


def solution(mesh):
    return jax.shard_map(
        functools.partial(body, mesh.shape["bank"], mesh.shape["freq"]),
        mesh=mesh,
        in_specs=(
            P(("groups", "seg", "bank"), None, "freq"),
            P(("groups", "seg", "bank"), None, "freq"),
            P(None, "bank", "freq"),
            P(None, "bank", None, "freq"),
            P(("groups", "freq")),
            P(("groups", "freq")),
            P(("groups", "seg"), None),
            P(("groups", "seg"), None),
        ),
        out_specs=(
            P(("bank", "freq"), ("groups", "seg")),
            P(("groups", "seg", "bank"), None, "freq"),
        ),
        check_vma=False,
    )
```

```python
import functools
import math

import jax
import jax.numpy as jnp
from jax import lax
from jax.experimental import pallas as pl
from jax.experimental.pallas import tpu as pltpu
from jax.sharding import PartitionSpec as P

FC = 16384
FB = 65536
CAP = 2
LC = 16
LF = 16
CSTRIDE = 2047
PERIOD = 131072
STEP = 512
DEEP = 2048
LANES = 128
MESH = pl.DeviceIdType.MESH
NT = (((1,), (1,)), ((), ()))
NN = (((1,), (0,)), ((), ()))


def unit_phase(count):
    quadrant = (count + PERIOD // 8) >> 15
    x = (count - (quadrant << 15)).astype(jnp.float32) * (2.0 * math.pi / PERIOD)
    z = x * x
    s = x * (1.0 + z * (-1.0 / 6 + z * (1.0 / 120 + z * (-1.0 / 5040 + z * (1.0 / 362880)))))
    c = 1.0 + z * (-0.5 + z * (1.0 / 24 + z * (-1.0 / 720 + z * (1.0 / 40320 - z * (1.0 / 3628800)))))
    odd = (quadrant & 1) == 1
    cos = jnp.where(odd, s, c)
    sin = jnp.where(odd, c, s)
    cos = jnp.where(((quadrant + 1) & 2) == 2, -cos, cos)
    sin = jnp.where((quadrant & 2) == 2, -sin, sin)
    return cos, sin


def kernel(
    nb,
    nf,
    marks,
    cs_hbm,
    fs_hbm,
    ct_hbm,
    ft_hbm,
    cw_hbm,
    fw_hbm,
    coarse_out,
    fine_out,
    craw,
    fraw,
    cbuf,
    fbuf,
    ct,
    ft,
    cw,
    fw,
    cpure,
    fpure,
    ctab,
    ftab,
    clag,
    flag,
    cpq,
    fpq,
    sel,
    soff,
    cstage,
    crecv,
    fstage,
    frecv,
    nstage,
    nrecv,
    cnorm,
    fnorm,
    cres,
    rstage,
    rrecv,
    load_sem,
    w_sem,
    ct_sem,
    ft_sem,
    c_send,
    c_recv,
    f_send,
    f_recv,
    n_send,
    n_recv,
    cx_send,
    cx_recv,
    fx_send,
    fx_recv,
    r_send,
    r_recv,
):
    me = lax.axis_index("bank")
    fx = lax.axis_index("freq")
    groups = nb // 4
    segs = cbuf.shape[1] // 2
    cbins = cbuf.shape[2]
    fbins = fbuf.shape[2]
    parts = f_send.shape[1]
    fpart = fbins // parts
    ctn = ct.shape[0] // 2
    ftn = ft.shape[0] // 2
    cq = ctn // nf
    fq = ftn // nf
    scale = PERIOD // (2 * FC)
    shift_bits = nb.bit_length() - 1

    def source(p):
        step = (nb - (p + 1) // 2) if p % 2 else p // 2
        return lax.rem(me + step, nb)

    def other(k):
        return lax.rem(fx + k, nf)

    right = lax.rem(me + 1, nb)
    left = lax.rem(me + nb - 1, nb)

    def c_move(p):
        return pltpu.make_async_remote_copy(
            src_ref=cbuf.at[max(p - 2, 0)],
            dst_ref=cbuf.at[p],
            send_sem=c_send.at[p],
            recv_sem=c_recv.at[p],
            device_id={"bank": right if p % 2 else left},
            device_id_type=MESH,
        )

    def f_move(p, c, leftward=None):
        if leftward is None:
            leftward = p % 2 == 0
        origin = p - 1 if (p == nb - 1 and leftward) else max(p - 2, 0)
        part = pl.ds(pl.multiple_of(c * fpart, fpart), fpart)
        return pltpu.make_async_remote_copy(
            src_ref=fbuf.at[origin, :, part],
            dst_ref=fbuf.at[p, :, part],
            send_sem=f_send.at[p, c],
            recv_sem=f_recv.at[p, c],
            device_id={"bank": left if leftward else right},
            device_id_type=MESH,
        )

    def n_move(k):
        return pltpu.make_async_remote_copy(
            src_ref=nstage.at[other(k)],
            dst_ref=nrecv.at[k - 1],
            send_sem=n_send.at[k - 1],
            recv_sem=n_recv.at[k - 1],
            device_id={"freq": other(k)},
            device_id_type=MESH,
        )

    def cx_move(g, k):
        return pltpu.make_async_remote_copy(
            src_ref=cstage.at[g, other(k)],
            dst_ref=crecv.at[g, k - 1],
            send_sem=cx_send.at[g, k - 1],
            recv_sem=cx_recv.at[g, k - 1],
            device_id={"freq": other(k)},
            device_id_type=MESH,
        )

    def fx_move(g, k):
        return pltpu.make_async_remote_copy(
            src_ref=fstage.at[g, other(k)],
            dst_ref=frecv.at[g, k - 1],
            send_sem=fx_send.at[g, k - 1],
            recv_sem=fx_recv.at[g, k - 1],
            device_id={"freq": other(k)},
            device_id_type=MESH,
        )

    def r_move(p):
        return pltpu.make_async_remote_copy(
            src_ref=rstage.at[p // 4 if p < nb - 1 else groups],
            dst_ref=rrecv.at[p],
            send_sem=r_send.at[p],
            recv_sem=r_recv.at[p],
            device_id={"bank": source(p)},
            device_id_type=MESH,
        )

    own_c = pltpu.make_async_copy(cs_hbm, craw, load_sem.at[0])

    def own_f(c):
        part = pl.ds(c * fpart, fpart)
        return pltpu.make_async_copy(fs_hbm.at[:, :, part], fraw.at[:, :, part], load_sem.at[c + 1])

    for c in range(parts):
        own_f(c).start()
    own_c.start()
    load_cw = pltpu.make_async_copy(cw_hbm, cw, w_sem.at[0])
    load_fw = pltpu.make_async_copy(fw_hbm, fw, w_sem.at[1])
    load_cw.start()
    load_fw.start()
    load_ct = pltpu.make_async_copy(ct_hbm, ct, ct_sem)
    load_ft = pltpu.make_async_copy(ft_hbm, ft, ft_sem)

    barrier = pltpu.get_barrier_semaphore()
    for neighbour in (left, right):
        pl.semaphore_signal(barrier, inc=1, device_id={"bank": neighbour}, device_id_type=MESH)
    for k in range(1, nf):
        pl.semaphore_signal(barrier, inc=1, device_id={"freq": other(k)}, device_id_type=MESH)

    def settle(raw, buf, begin, size):
        for at in range(begin, begin + size, STEP):
            piece = [raw[r, :, at : at + STEP].astype(jnp.float32) for r in range(segs)]
            buf[0, :, at : at + STEP] = jnp.concatenate(piece, axis=0).astype(jnp.bfloat16)

    own_f(0).wait()
    settle(fraw, fbuf, 0, fpart)
    pl.semaphore_wait(barrier, 2 + nf - 1)
    for c in range(parts):
        if c + 1 < parts:
            own_f(c + 1).wait()
            settle(fraw, fbuf, (c + 1) * fpart, fpart)
        else:
            own_c.wait()
            settle(craw, cbuf, 0, cbins)
        for p in (1, 2):
            f_move(p, c).start()
    for p in (1, 2):
        c_move(p).start()
    load_ct.start()
    load_ft.start()
    load_cw.wait()
    load_fw.wait()

    def c_phases(i, carry):
        at = pl.ds(pl.multiple_of(i * STEP, STEP), STEP)
        lag = lax.broadcasted_iota(jnp.int32, (LC, STEP), 0) * CSTRIDE
        f = fx * cbins + i * STEP + lax.broadcasted_iota(jnp.int32, (LC, STEP), 1)
        cos, sin = unit_phase((f * lag * scale) & (PERIOD - 1))
        w = cw[:, at]
        ctab[0, :, at] = cos * w
        ctab[1, :, at] = sin * w
        return carry

    lax.fori_loop(0, cbins // STEP, c_phases, 0)

    def f_phases(i, carry):
        at = pl.ds(pl.multiple_of(i * STEP, STEP), STEP)
        lag = lax.broadcasted_iota(jnp.int32, (LF, STEP), 0)
        f = fx * fbins + i * STEP + lax.broadcasted_iota(jnp.int32, (LF, STEP), 1)
        cos, sin = unit_phase((f * lag) & (PERIOD - 1))
        w = fw[:, at]
        ftab[0, :, at] = cos * w
        ftab[1, :, at] = sin * w
        return carry

    lax.fori_loop(0, fbins // STEP, f_phases, 0)

    rows = lax.broadcasted_iota(jnp.int32, (16, 8 * segs), 0)
    cols = lax.broadcasted_iota(jnp.int32, (16, 8 * segs), 1)
    orow = lax.broadcasted_iota(jnp.int32, (8, LANES), 0)
    units = [list(range(4 * g, min(4 * g + 4, nb - 1))) for g in range(groups)] + [[nb - 1]]
    for u, places in enumerate(units):
        pick = jnp.zeros((16, 8 * segs), jnp.float32)
        shift = jnp.zeros((8, LANES), jnp.int32)
        for i, p in enumerate(places):
            base = source(p) * segs
            found = jnp.int32(0)
            for s in range(segs):
                for k in range(2):
                    mark = marks[k, base + s]
                    hit = jnp.where((mark & (nb - 1)) == me, 1, 0)
                    slot = 2 * i + found
                    row = (rows & 7) >> 2 if u == groups else rows & 7
                    col = (i * segs + s) * 2
                    here = (row == slot) & (cols == col + (rows >> 3))
                    pick += jnp.where(here, hit.astype(jnp.float32), 0.0)
                    shift += jnp.where((orow >> 2 if u == groups else orow) == slot, hit * (mark >> shift_bits), 0)
                    found = found + hit
        sel[u] = pick.astype(jnp.bfloat16)
        soff[u] = shift

    def powers():
        load_ct.wait()

        def c_power(i, total):
            at = pl.ds(pl.multiple_of(i * LANES, LANES), LANES)
            re = ct[:ctn, at].astype(jnp.float32)
            im = ct[ctn:, at].astype(jnp.float32)
            return total + (re * re + im * im) * cw[:, at]

        ct_sum = lax.fori_loop(0, cbins // LANES, c_power, jnp.zeros((ctn, LANES), jnp.float32), unroll=2)
        ct_sum = jnp.broadcast_to(jnp.sum(ct_sum, axis=1, keepdims=True), (ctn, LANES))
        load_ft.wait()

        def f_power(i, total):
            at = pl.ds(pl.multiple_of(i * LANES, LANES), LANES)
            re = ft[:ftn, at].astype(jnp.float32)
            im = ft[ftn:, at].astype(jnp.float32)
            return total + (re * re + im * im) * fw[:, at]

        ft_sum = lax.fori_loop(0, fbins // LANES, f_power, jnp.zeros((ftn, LANES), jnp.float32), unroll=4)
        ft_sum = jnp.broadcast_to(jnp.sum(ft_sum, axis=1, keepdims=True), (ftn, LANES))
        for q in range(nf):
            nstage[q, :cq] = ct_sum[q * cq : (q + 1) * cq]
            nstage[q, cq:] = ft_sum[q * fq : (q + 1) * fq]

    def coarse_group(g):
        half = 4 * segs
        prow = lax.broadcasted_iota(jnp.int32, (2 * half, 2 * half), 0)
        pcol = lax.broadcasted_iota(jnp.int32, (2 * half, 2 * half), 1)
        want = jnp.where(prow < half, 2 * prow, 2 * (prow - half) + 1)
        split = jnp.where(pcol == want, 1.0, 0.0).astype(jnp.bfloat16)
        ncol = LC * half
        wide = min(2 * STEP, cbins)
        for begin in range(0, cbins, wide):
            at = slice(begin, begin + wide)
            block = jnp.concatenate([cbuf[4 * g + b, :, at].astype(jnp.float32) for b in range(4)], axis=0)
            cpure[:, at] = lax.dot_general(split, block.astype(jnp.bfloat16), NN, preferred_element_type=jnp.float32)
        cpq[...] = jnp.zeros_like(cpq)
        deep = min(DEEP, cbins)

        def step(i, carry):
            base = pl.multiple_of(i * deep, deep)
            for kt in range(0, deep, 2 * LANES):
                at = pl.ds(base + kt, 2 * LANES)
                yr, yi = cpure[:half, at], cpure[half:, at]
                for j in range(LC):
                    c = ctab[0, j : j + 1, at]
                    s = ctab[1, j : j + 1, at]
                    clag[j * half : (j + 1) * half, kt : kt + 2 * LANES] = (yr * c - yi * s).astype(jnp.bfloat16)
                    clag[ncol + j * half : ncol + (j + 1) * half, kt : kt + 2 * LANES] = (yr * s + yi * c).astype(jnp.bfloat16)
            cpq[...] += lax.dot_general(clag[...], ct[:, pl.ds(base, deep)], NT, preferred_element_type=jnp.float32)
            return carry

        lax.fori_loop(0, cbins // deep, step, 0)
        re = (cpq[:ncol, :ctn] + cpq[ncol:, ctn:]).T
        im = (cpq[ncol:, :ctn] - cpq[:ncol, ctn:]).T
        for q in range(nf):
            cstage[g, q, :cq] = re[q * cq : (q + 1) * cq]
            cstage[g, q, cq:] = im[q * cq : (q + 1) * cq]

    def fine_piece(u, c):
        single = u == groups
        ncol = LF * (2 if single else 8)
        low = lax.broadcasted_iota(jnp.int32, (8, 2 * LANES), 0) < 4
        places = units[u] + (units[groups - 1] if single else [])
        places = (places + places)[:4]
        wide = min(2 * STEP, fpart)
        for begin in range(0, fpart, wide):
            first = c * fpart + begin
            at = pl.ds(pl.multiple_of(first, wide), wide)
            block = jnp.concatenate([fbuf[p, :, at].astype(jnp.float32) for p in places], axis=0)
            y = lax.dot_general(sel[u], block.astype(jnp.bfloat16), NN, preferred_element_type=jnp.float32)
            f = fx * fbins + first + lax.broadcasted_iota(jnp.int32, (8, wide), 1)
            shift = jnp.concatenate([soff[u]] * (wide // LANES), axis=1)
            cos, sin = unit_phase((f * shift) & (PERIOD - 1))
            yr, yi = y[:8], y[8:]
            fpure[:8, begin : begin + wide] = yr * cos - yi * sin
            fpure[8:, begin : begin + wide] = yr * sin + yi * cos
        deep = fpart if single else min(DEEP, fpart)

        def step(i, carry):
            base = pl.multiple_of(i * deep, deep)
            whole = pl.multiple_of(c * fpart + i * deep, deep)
            for kt in range(0, deep, 2 * LANES):
                sr = fpure[:8, pl.ds(base + kt, 2 * LANES)]
                si = fpure[8:, pl.ds(base + kt, 2 * LANES)]
                at = pl.ds(whole + kt, 2 * LANES)
                here = slice(kt, kt + 2 * LANES)
                for j in range(0, ncol // 8, 2):
                    if single:
                        pair = []
                        for part in range(2):
                            rows8 = ftab[part, j * 4 : j * 4 + 8, at]
                            turned = pltpu.roll(rows8, 4, 0)
                            pair.append((jnp.where(low, rows8, turned), jnp.where(low, turned, rows8)))
                    res, ims = [], []
                    for jj in range(2):
                        if single:
                            wc, ws = pair[0][jj], pair[1][jj]
                        else:
                            wc = ftab[0, j + jj : j + jj + 1, at]
                            ws = ftab[1, j + jj : j + jj + 1, at]
                        res.append(sr * wc - si * ws)
                        ims.append(sr * ws + si * wc)
                    flag[j * 8 : j * 8 + 16, here] = jnp.concatenate(res, axis=0).astype(jnp.bfloat16)
                    flag[ncol + j * 8 : ncol + j * 8 + 16, here] = jnp.concatenate(ims, axis=0).astype(jnp.bfloat16)
            fpq[: 2 * ncol] += lax.dot_general(
                flag[: 2 * ncol, :deep], ft[:, pl.ds(whole, deep)], NT, preferred_element_type=jnp.float32
            )
            return carry

        lax.fori_loop(0, fpart // deep, step, 0)

    def fine_done(u):
        ncol = LF * (2 if u == groups else 8)
        top, bottom = fpq[:ncol], fpq[ncol : 2 * ncol]
        re = top + pltpu.roll(bottom, ftn, 1)
        im = bottom - pltpu.roll(top, ftn, 1)
        if ncol < LANES:
            rest = jnp.zeros((LANES - ncol, LANES), jnp.float32)
            re = jnp.concatenate([re, rest], axis=0)
            im = jnp.concatenate([im, rest], axis=0)
        re, im = re.T, im.T
        for q in range(nf):
            fstage[u, q, :fq] = re[q * fq : (q + 1) * fq]
            fstage[u, q, fq:] = im[q * fq : (q + 1) * fq]

    def coarse_peak(g):
        total = cstage[g, fx]
        for k in range(1, nf):
            cx_move(g, k).wait_recv()
            total = total + crecv[g, k - 1]
        energy = total[:cq] * total[:cq] + total[cq:] * total[cq:]
        half = 4 * segs
        peak = energy[:, :LANES]
        for b in range(1, LC * half // LANES):
            peak = jnp.maximum(peak, energy[:, b * LANES : (b + 1) * LANES])
        span = LANES // 2
        while span >= half:
            peak = jnp.maximum(peak, pltpu.roll(peak, span, 1))
            span //= 2
        peak = peak / cnorm[...]
        lane = lax.broadcasted_iota(jnp.int32, (cq, LANES), 1) // segs
        for i in range(4):
            src = source(4 * g + i)
            moved = pltpu.roll(peak, lax.rem(src * segs + LANES - i * segs, LANES), 1)
            cres[...] = jnp.where(lane == src, moved, cres[...])

    def fine_peak(g):
        total = fstage[g, fx]
        for k in range(1, nf):
            fx_move(g, k).wait_recv()
            total = total + frecv[g, k - 1]
        energy = total[:fq] * total[:fq] + total[fq:] * total[fq:]
        peak = energy
        for span in (16, 8, 2, 1) if g == groups else (64, 32, 16, 8):
            peak = jnp.maximum(peak, pltpu.roll(peak, LANES - span, 1))
        peak = peak / fnorm[...]
        square = jnp.concatenate([peak, jnp.zeros((LANES - fq, LANES), jnp.float32)], axis=0)
        rstage[g] = square.T[:8]

    def norms():
        total = nstage[fx]
        for k in range(1, nf):
            n_move(k).wait_recv()
            total = total + nrecv[k - 1]
        cnorm[...] = total[:cq]
        fnorm[...] = total[cq:]
        cres[...] = jnp.zeros_like(cres)

    def give_back(u):
        for p in units[u]:
            if p > 0:
                r_move(p).start()

    def start_all(move, g):
        for k in range(1, nf):
            move(g, k).start()

    def hop(h, unit=None, first=None):
        here = [p for p in (2 * h - 1, 2 * h) if p <= nb - 1]
        half = parts // 2
        if unit is not None:
            fpq[...] = jnp.zeros_like(fpq)

        def part(i, carry):
            c = (i % 2) * half + i // 2 if here == [nb - 1] else i
            for p in here:
                f_move(p, c).wait_recv()
                if p + 2 < nb - 1:
                    f_move(p + 2, c).start()
                elif p + 2 == nb - 1:

                    @pl.when(c < half)
                    def _():
                        f_move(nb - 1, c, leftward=False).start()

                elif p + 1 == nb - 1:

                    @pl.when(c >= half)
                    def _():
                        f_move(nb - 1, c, leftward=True).start()

            if first is not None:

                @pl.when(i == 0)
                def _():
                    first()

            if unit is not None:
                fine_piece(unit, c)
            return carry

        lax.fori_loop(0, parts, part, 0)
        if unit is not None:
            fine_done(unit)
            start_all(fx_move, unit)

    def pass_coarse(h):
        for p in (2 * h - 1, 2 * h):
            if p <= nb - 1:
                c_move(p).wait_recv()
                if p + 2 <= nb - 1:
                    c_move(p + 2).start()

    if groups == 1:
        powers()
        for k in range(1, nf):
            n_move(k).start()
    for g in range(groups - 1):
        hop(2 * g + 1, first=functools.partial(start_all, cx_move, g - 1) if g else None)
        pass_coarse(2 * g + 1)
        if g == 0:
            powers()
        else:
            if g == 1:
                norms()
            fine_peak(g - 1)
            give_back(g - 1)
            coarse_peak(g - 1)
        hop(2 * g + 2, g)
        pass_coarse(2 * g + 2)
        if g == 0:
            for k in range(1, nf):
                n_move(k).start()
        coarse_group(g)
    last = groups - 1
    hop(2 * last + 1, last, functools.partial(start_all, cx_move, last - 1) if last else None)
    pass_coarse(2 * last + 1)
    hop(2 * last + 2, groups)
    if groups <= 2:
        norms()
    pass_coarse(2 * last + 2)
    coarse_group(last)
    start_all(cx_move, last)
    if last:
        fine_peak(last - 1)
        give_back(last - 1)
    fine_peak(last)
    give_back(last)
    fine_peak(groups)
    give_back(groups)
    rrecv[0] = rstage[0]
    if last:
        coarse_peak(last - 1)

    spots, named = [], []
    for s in range(segs):
        for k in range(2):
            bank = marks[k, me * segs + s] & (nb - 1)
            rank = jnp.int32(0)
            for before in named:
                rank = rank + jnp.where(before == bank, 1, 0)
            named.append(bank)
            away = lax.rem(me - bank + nb, nb)
            place = jnp.where(away < nb // 2, 2 * away, 2 * (nb - away) - 1)
            row = jnp.where(place == nb - 1, 4 * rank, lax.rem(place, 4) * 2 + rank)
            spots.append((jnp.clip(place, 0, nb - 1), jnp.clip(row, 0, 7)))
    for p in range(1, nb):
        c_move(p).wait_send()
        for c in range(parts):
            f_move(p, c).wait_send()
    for k in range(1, nf):
        n_move(k).wait_send()
        for g in range(groups + 1):
            fx_move(g, k).wait_send()
            if g < last:
                cx_move(g, k).wait_send()
    for p in range(1, nb - 4):
        r_move(p).wait_send()
    coarse_peak(last)
    coarse_out[...] = cres[...]
    for k in range(1, nf):
        cx_move(last, k).wait_send()
    for p in range(max(1, nb - 4), nb):
        r_move(p).wait_send()
    for p in range(1, nb):
        r_move(p).wait_recv()
    result = jnp.zeros((8, LANES), jnp.float32)
    for n, (place, row) in enumerate(spots):
        line = rrecv[place, pl.ds(row, 1), :]
        result = jnp.where(orow == n, line, result)
    fine_out[...] = result


def body(
    nb,
    nf,
    coarse_spectra,
    fine_spectra,
    coarse_templates,
    fine_templates,
    coarse_weight,
    fine_weight,
    triggers,
    offsets,
):
    segs, _, cbins = coarse_spectra.shape
    fbins = fine_spectra.shape[2]
    ctn = coarse_templates.shape[1]
    ftn = fine_templates.shape[2]
    groups = nb // 4
    parts = 4
    cq, fq = ctn // nf, ftn // nf
    ccol, fcol = LC * 4 * segs, LF * 8
    f32, bf16 = jnp.float32, jnp.bfloat16
    dma = pltpu.SemaphoreType.DMA
    anywhere = pl.BlockSpec(memory_space=pl.ANY)
    smem = pl.BlockSpec(memory_space=pltpu.SMEM)
    vmem = pl.BlockSpec(memory_space=pltpu.VMEM)
    coarse, fine = pl.pallas_call(
        functools.partial(kernel, nb, nf),
        out_shape=(
            jax.ShapeDtypeStruct((cq, LANES), f32),
            jax.ShapeDtypeStruct((8, LANES), f32),
        ),
        in_specs=[smem] + [anywhere] * 6,
        out_specs=(vmem, vmem),
        scratch_shapes=[
            pltpu.VMEM((segs, 2, cbins), bf16),
            pltpu.VMEM((segs, 2, fbins), bf16),
            pltpu.VMEM((nb, 2 * segs, cbins), bf16),
            pltpu.VMEM((nb, 2 * segs, fbins), bf16),
            pltpu.VMEM((2 * ctn, cbins), bf16),
            pltpu.VMEM((2 * ftn, fbins), bf16),
            pltpu.VMEM((1, cbins), f32),
            pltpu.VMEM((1, fbins), f32),
            pltpu.VMEM((8 * segs, cbins), f32),
            pltpu.VMEM((16, fbins // parts), f32),
            pltpu.VMEM((2, LC, cbins), f32),
            pltpu.VMEM((2, LF, fbins), f32),
            pltpu.VMEM((2 * ccol, min(DEEP, cbins)), bf16),
            pltpu.VMEM((2 * fcol, fbins // parts), bf16),
            pltpu.VMEM((2 * ccol, 2 * ctn), f32),
            pltpu.VMEM((2 * fcol, 2 * ftn), f32),
            pltpu.VMEM((groups + 1, 16, 8 * segs), bf16),
            pltpu.VMEM((groups + 1, 8, LANES), jnp.int32),
            pltpu.VMEM((groups, nf, 2 * cq, ccol), f32),
            pltpu.VMEM((groups, nf - 1, 2 * cq, ccol), f32),
            pltpu.VMEM((groups + 1, nf, 2 * fq, fcol), f32),
            pltpu.VMEM((groups + 1, nf - 1, 2 * fq, fcol), f32),
            pltpu.VMEM((nf, cq + fq, LANES), f32),
            pltpu.VMEM((nf - 1, cq + fq, LANES), f32),
            pltpu.VMEM((cq, LANES), f32),
            pltpu.VMEM((fq, LANES), f32),
            pltpu.VMEM((cq, LANES), f32),
            pltpu.VMEM((groups + 1, 8, LANES), f32),
            pltpu.VMEM((nb, 8, LANES), f32),
            dma((parts + 1,)),
            dma((2,)),
            dma,
            dma,
            dma((nb,)),
            dma((nb,)),
            dma((nb, parts)),
            dma((nb, parts)),
            dma((nf - 1,)),
            dma((nf - 1,)),
            dma((groups, nf - 1)),
            dma((groups, nf - 1)),
            dma((groups + 1, nf - 1)),
            dma((groups + 1, nf - 1)),
            dma((nb,)),
            dma((nb,)),
        ],
        compiler_params=pltpu.CompilerParams(
            collective_id=0, has_side_effects=True, vmem_limit_bytes=55200 * 1024
        ),
        name="search",
    )(
        (offsets * nb + triggers).T,
        coarse_spectra,
        fine_spectra,
        coarse_templates.reshape(2 * ctn, cbins),
        fine_templates.reshape(2 * ftn, fbins),
        coarse_weight.reshape(1, cbins),
        fine_weight.reshape(1, fbins),
    )
    coarse_snr = coarse[:, : nb * segs]
    fine_snr = fine[:, :fq].reshape(segs, 2, fq)
    return coarse_snr, fine_snr


def solution(mesh):
    return jax.shard_map(
        functools.partial(body, mesh.shape["bank"], mesh.shape["freq"]),
        mesh=mesh,
        in_specs=(
            P(("groups", "seg", "bank"), None, "freq"),
            P(("groups", "seg", "bank"), None, "freq"),
            P(None, "bank", "freq"),
            P(None, "bank", None, "freq"),
            P(("groups", "freq")),
            P(("groups", "freq")),
            P(("groups", "seg"), None),
            P(("groups", "seg"), None),
        ),
        out_specs=(
            P(("bank", "freq"), ("groups", "seg")),
            P(("groups", "seg", "bank"), None, "freq"),
        ),
        check_vma=False,
    )
```
